128 devices in a mesh: rep: 2 (over core), dp: 64 (over x, y, z).
Axes of the slice: x: 4, y: 4, z: 4, core: 2. Of those that a mesh axis runs over, the one named last changes fastest.
Arguments:
- g_w_gate: bfloat16 [128, 2, 640, 2048], P(('rep', 'dp')), parts along dimension 0
- g_w_up: bfloat16 [128, 2, 640, 2048], P(('rep', 'dp')), parts along dimension 0
- g_w_down: bfloat16 [128, 2, 2048, 640], P(('rep', 'dp')), parts along dimension 0
- w_gate: bfloat16 [2, 640, 2048], replicated
- w_up: bfloat16 [2, 640, 2048], replicated
- w_down: bfloat16 [2, 2048, 640], replicated
- m_w_gate: float32 [2, 640, 2048], P(None, 'dp')
- m_w_up: float32 [2, 640, 2048], P(None, 'dp')
- m_w_down: float32 [2, 2048, 640], P(None, 'dp')
- v_w_gate: float32 [2, 640, 2048], P(None, 'dp')
- v_w_up: float32 [2, 640, 2048], P(None, 'dp')
- v_w_down: float32 [2, 2048, 640], P(None, 'dp')
Outputs:
- output 1: bfloat16 [4, 640, 2048], P('rep'), parts along dimension 0
- output 2: bfloat16 [4, 640, 2048], P('rep'), parts along dimension 0
- output 3: bfloat16 [4, 2048, 640], P('rep'), parts along dimension 0
- output 4: float32 [4, 640, 2048], P('rep', 'dp'), parts along dimension 0
- output 5: float32 [4, 640, 2048], P('rep', 'dp'), parts along dimension 0
- output 6: float32 [4, 2048, 640], P('rep', 'dp'), parts along dimension 0
- output 7: float32 [4, 640, 2048], P('rep', 'dp'), parts along dimension 0
- output 8: float32 [4, 640, 2048], P('rep', 'dp'), parts along dimension 0
- output 9: float32 [4, 2048, 640], P('rep', 'dp'), parts along dimension 0
There are 2 independent parts. The reference program is written for one: setup_inputs(seed, part) draws one part's arguments, and reference() takes and returns one part's arrays. A program takes and returns all parts, laid end to end along the dimension named above; an argument that names none is the same for every part.
All inputs are finite; a program needn't handle non-finite values.
Results may differ from the reference program's by a relative error of at most 0.022.
Values are sent between devices in bfloat16 or wider.
A program may use at most 1.5 GiB of HBM per device.

```python
import jax
import jax.numpy as jnp
from jax import lax

DEVICES = 64
D = 640
FF = 2048
LAYERS = 2
NAMES = ("w_gate", "w_up", "w_down")
SHAPES = {"w_gate": (LAYERS, D, FF), "w_up": (LAYERS, D, FF), "w_down": (LAYERS, FF, D)}


def setup_inputs(seed: int = 0, part: int = 0) -> dict:
    kz, *keys = jax.random.split(jax.random.key(seed), 1 + 5 * len(NAMES))
    loud = 2.0 ** jax.random.uniform(kz, (), jnp.float32, -1.0, 1.0)
    drawn = {}
    for name, key, both in zip(NAMES, keys[:3], keys[3:6], strict=True):
        own = jax.random.normal(jax.random.fold_in(key, part), (DEVICES, *SHAPES[name]), jnp.float32)
        shared = jax.random.normal(jax.random.fold_in(both, part), SHAPES[name], jnp.float32)
        drawn["g_" + name] = (loud * (0.7 * shared / DEVICES + 0.7 * own * DEVICES**-0.5)).astype(jnp.bfloat16)
    for name, key in zip(NAMES, keys[6:9], strict=True):
        drawn[name] = (jax.random.normal(key, SHAPES[name], jnp.float32) * SHAPES[name][1] ** -0.5).astype(jnp.bfloat16)
    for name, key in zip(NAMES, keys[9:12], strict=True):
        drawn["m_" + name] = loud * 0.5 * jax.random.normal(key, SHAPES[name], jnp.float32)
    for name, key in zip(NAMES, keys[12:15], strict=True):
        drawn["v_" + name] = loud * loud * jax.random.uniform(key, SHAPES[name], jnp.float32, 0.5, 1.5)
    return drawn


def adamw(w, m, v, g):
    m = 0.9 * m + 0.1 * g
    v = 0.95 * v + 0.05 * g * g
    step = m * lax.rsqrt(v + 1e-8) + 0.1 * w
    return (w - 0.02 * step).astype(jnp.bfloat16), m, v


def reference(g_w_gate, g_w_up, g_w_down, w_gate, w_up, w_down, m_w_gate, m_w_up, m_w_down, v_w_gate, v_w_up, v_w_down):
    def total(terms):
        return lax.scan(lambda so_far, term: (so_far + term.astype(jnp.float32), None), jnp.zeros(terms.shape[1:], jnp.float32), terms)[0]

    gradients = [total(terms).astype(jnp.bfloat16).astype(jnp.float32) for terms in (g_w_gate, g_w_up, g_w_down)]
    new = [
        adamw(w.astype(jnp.float32), m, v, g)
        for w, m, v, g in zip((w_gate, w_up, w_down), (m_w_gate, m_w_up, m_w_down), (v_w_gate, v_w_up, v_w_down), gradients, strict=True)
    ]
    return tuple(one[which] for which in range(3) for one in new)
```

```python
import jax
import jax.numpy as jnp
from jax import lax
from jax.experimental import pallas as pl
from jax.experimental.pallas import tpu as pltpu
from jax.sharding import PartitionSpec as P

MESH = pl.DeviceIdType.MESH
F32, BF16 = jnp.float32, jnp.bfloat16
CHUNKS = 2
COLS = 2048 // CHUNKS
TILES = 4 // CHUNKS


class Piece:
    def __init__(self, weight, chunk):
        self.weight, self.chunk = weight, chunk
        if weight < 2:
            self.axes = ((0, 1, 2), (1, 0, 2))[weight]
            self.lead1, self.lead2, self.lead3 = (4, 5), (5,), (2,)
            self.cols = COLS
        else:
            self.axes = ((2, 0, 1), (2, 1, 0))[chunk % 2]
            self.lead1, self.lead2, self.lead3 = (4, 4, TILES), (4, TILES), (TILES,)
            self.cols = 640

    def shape(self, lead, *front):
        return (*front, *lead, 8, self.cols)

    def scratch(self):
        one, two, three = self.lead1, self.lead2, self.lead3
        shapes = [
            (self.shape(one, 2, 2), BF16),
            (self.shape(one, 3, 2), BF16),
            (self.shape(two, 2, 2), F32),
            (self.shape(two, 2, 2), BF16),
            (self.shape(two, 3, 2), BF16),
            (self.shape(two, 2), F32),
            (self.shape(two, 2), BF16),
            (self.shape(three, 3, 2), BF16),
        ]
        if self.weight < 2:
            shapes.append((self.shape(three, 4, 2), BF16))
        return shapes

    def columns(self):
        return pl.ds(self.chunk * COLS, COLS)

    def first(self, ref, layer, p):
        if self.weight == 0:
            return ref.at[layer, p, :, :, :, self.columns()]
        if self.weight == 1:
            return ref.at[layer, :, p, :, :, self.columns()]
        return ref.at[layer, :, :, p, pl.ds(self.chunk * TILES, TILES)]

    def second(self, block, p):
        if self.weight == 2 and self.axes[1] == 1:
            return block.at[:, p]
        return block.at[p]

    def third(self, block, p):
        return block.at[pl.ds(p, 2)] if self.weight < 2 else block.at[p]

    def out2(self, ref, layer, p, pos):
        if self.weight == 0:
            return ref.at[layer, pos[0], p, :, :, self.columns()]
        if self.weight == 1:
            return ref.at[layer, p, pos[1], :, :, self.columns()]
        rows = pl.ds(self.chunk * TILES, TILES)
        if self.axes[1] == 0:
            return ref.at[layer, p, :, pos[2], rows]
        return ref.at[layer, :, p, pos[2], rows]

    def out3(self, ref, layer, p, pos):
        rows = pl.ds(self.chunk * TILES, TILES)
        if self.axes[2] == 1:
            return ref.at[layer, pos[0], p, pos[2], rows]
        return ref.at[layer, p, pos[1], pos[2], rows]


PIECES = [Piece(w, c) for c in range(CHUNKS) for w in range(3)]
COPIES = 36 * len(PIECES)
LOADS = 4 * len(PIECES) + 9


def each_slab(lead, body):
    outer = 1
    for n in lead[:-1]:
        outer *= n

    def some(i):
        front = []
        for n in reversed(lead[:-1]):
            front.insert(0, lax.rem(i, n))
            i = lax.div(i, n)
        for j in range(lead[-1]):
            body((*front, j))

    if outer == 1:
        some(jnp.int32(0))
    else:
        lax.fori_loop(0, outer, lambda i, c: (some(i), c)[1], 0)


def add_into(lead, terms, outs):
    def body(index):
        total = terms[0][index].astype(F32)
        for t in terms[1:]:
            total = total + t[index].astype(F32)
        for o in outs:
            o[index] = total.astype(o.dtype)

    each_slab(lead, body)


def adamw(w, m, v, g):
    m = 0.9 * m + 0.1 * g
    v = 0.95 * v + 0.05 * g * g
    step = m * lax.rsqrt(v + 1e-8) + 0.1 * w
    return w - 0.02 * step, m, v


def kernel(*refs):
    refs = list(refs)

    def take(n):
        got, refs[:n] = refs[:n], []
        return got

    grads, weights, ms, vs = take(3), take(3), take(3), take(3)
    new_w, new_m, new_v = take(3), take(3), take(3)
    m_in, v_in, w_in = take(3), take(3), take(3)
    m_win, v_win = take(2), take(2)
    bufs = [take(len(p.scratch())) for p in PIECES]
    send_sem, recv_sem, load_sem = take(3)

    me = lax.axis_index("dp")
    pos = (lax.div(me, 16), lax.rem(lax.div(me, 4), 4), lax.rem(me, 4))
    stride = (16, 4, 1)

    def at(axis, d):
        return lax.rem(pos[axis] + d, 4)

    def neighbour(axis, d):
        return me + (at(axis, d) - pos[axis]) * stride[axis]

    plus = [neighbour(a, 1) for a in range(3)]
    minus = [neighbour(a, 3) for a in range(3)]

    barrier = pltpu.get_barrier_semaphore()
    for other in (*plus, *minus):
        pl.semaphore_signal(barrier, inc=1, device_id={"dp": other}, device_id_type=MESH)

    sent, loads = [], []

    def remote(src, dst, axis, forward):
        i = len(sent)
        copy = pltpu.make_async_remote_copy(
            src_ref=src,
            dst_ref=dst,
            send_sem=send_sem.at[i],
            recv_sem=recv_sem.at[i],
            device_id={"dp": (plus if forward else minus)[axis]},
            device_id_type=MESH,
        )
        sent.append(copy)
        copy.start()
        return copy

    def load(src, dst):
        copy = pltpu.make_async_copy(src, dst, load_sem.at[len(loads)])
        loads.append(copy)
        copy.start()
        return copy

    class Scatter:
        def __init__(self, axis, recv, far, near, lead, relay_term):
            self.axis, self.recv, self.far, self.near = axis, recv, far, near
            self.lead, self.relay_term = lead, relay_term
            self.got = {}

        def send_far(self):
            for layer in (0, 1):
                self.got["far", layer] = remote(self.far(layer), self.recv.at[0, layer], self.axis, layer == 0)

        def send_near(self):
            for layer in (1, 0):
                self.got["near", layer] = remote(self.near(layer), self.recv.at[1, layer], self.axis, layer == 1)

        def relay(self):
            for layer in (0, 1):
                self.got["far", layer].wait_recv()
                here = self.recv.at[0, layer]
                add_into(self.lead, (here, self.relay_term(layer)), (here,))
                self.got["relay", layer] = remote(here, self.recv.at[2, layer], self.axis, layer == 0)

        def wait(self, layer):
            self.got["near", layer].wait_recv()
            self.got["relay", layer].wait_recv()

    class Gather:
        def __init__(self, axis, block):
            self.axis, self.block = axis, block
            self.got = {}

        def send(self, layer, p, forward, key):
            ref = self.block(layer, p)
            self.got[key] = remote(ref, ref, self.axis, forward)

        def start(self):
            mine = pos[self.axis]
            self.send(0, mine, True, "from minus 0")
            self.send(1, mine, False, "from plus 1")
            self.send(1, mine, True, "from minus 1")
            self.send(0, mine, False, "from plus 0")

        def forward(self):
            self.got["from minus 0"].wait_recv()
            self.send(0, at(self.axis, 3), True, "far 0")
            self.got["from plus 1"].wait_recv()
            self.send(1, at(self.axis, 1), False, "far 1")

        def finish(self):
            for key in ("from minus 1", "from plus 0", "far 0", "far 1"):
                self.got[key].wait_recv()

    class Flow:
        def __init__(self, piece, buf):
            self.piece, self.buf = piece, buf
            a1, a2, a3 = piece.axes
            g = grads[piece.weight]
            own1, recv1, sum1, send1, recv2, sum2, send2, recv3 = buf[:8]
            self.scatter1 = Scatter(
                a1,
                recv1,
                lambda layer: piece.first(g, layer, at(a1, 2)),
                lambda layer: piece.first(g, layer, at(a1, 1 if layer else 3)),
                piece.lead1,
                lambda layer: own1.at[layer, 1],
            )
            self.scatter2 = Scatter(
                a2,
                recv2,
                lambda layer: send1.at[layer, 0],
                lambda layer: send1.at[layer, 1],
                piece.lead2,
                lambda layer: sum1.at[layer, 1],
            )
            self.scatter3 = Scatter(
                a3,
                recv3,
                lambda layer: piece.third(send2.at[layer], at(a3, 2)),
                lambda layer: piece.third(send2.at[layer], at(a3, 1 if layer else 3)),
                piece.lead3,
                lambda layer: piece.third(sum2.at[layer], at(a3, 3 if layer else 1)),
            )
            w = new_w[piece.weight]
            if piece.weight < 2:
                windows = buf[8]
                self.gather3 = Gather(a3, lambda layer, p: windows.at[p, layer])
            else:
                self.gather3 = Gather(a3, lambda layer, p: piece.out3(w, layer, p, pos))
            self.gather2 = Gather(a2, lambda layer, p: piece.out2(w, layer, p, pos))
            self.gather1 = Gather(a1, lambda layer, p: piece.first(w, layer, p))

        def load(self):
            piece, own1 = self.piece, self.buf[0]
            a1, g = piece.axes[0], grads[piece.weight]
            self.loaded = [[None, None], [None, None]]
            for which in (1, 0):
                for layer in (0, 1):
                    p = at(a1, (3 if layer else 1) if which else 0)
                    self.loaded[layer][which] = load(piece.first(g, layer, p), own1.at[layer, which])

        def far1(self):
            self.scatter1.send_far()

        def near1(self):
            self.scatter1.send_near()

        def relay1(self):
            for layer in (0, 1):
                self.loaded[layer][1].wait()
            self.scatter1.relay()

        def sum1(self):
            piece = self.piece
            own1, recv1, sum1, send1 = self.buf[:4]
            a2 = piece.axes[1]
            for layer in (0, 1):
                self.loaded[layer][0].wait()
                self.scatter1.wait(layer)

            def reduce(layer, d, out):
                p = at(a2, d)
                terms = (own1.at[layer, 0], recv1.at[1, layer], recv1.at[2, layer])
                add_into(piece.lead2, [piece.second(t, p) for t in terms], (out,))

            for layer in (0, 1):
                reduce(layer, 2, send1.at[layer, 0])
            self.scatter2.send_far()
            for layer in (1, 0):
                reduce(layer, 1 if layer else 3, send1.at[layer, 1])
            self.scatter2.send_near()
            for layer in (0, 1):
                reduce(layer, 3 if layer else 1, sum1.at[layer, 1])
            for layer in (0, 1):
                reduce(layer, 0, sum1.at[layer, 0])

        def relay2(self):
            self.scatter2.relay()

        def sum2(self):
            sum1, _, recv2, sum2, send2 = self.buf[2:7]
            for layer in (0, 1):
                self.scatter2.wait(layer)
                terms = (sum1.at[layer, 0], recv2.at[1, layer], recv2.at[2, layer])
                add_into(self.piece.lead2, terms, (sum2.at[layer], send2.at[layer]))
            self.scatter3.send_far()
            self.scatter3.send_near()

        def relay3(self):
            self.scatter3.relay()

        def step(self):
            piece = self.piece
            sum2, recv3 = self.buf[5], self.buf[7]
            a3, k = piece.axes[2], piece.weight
            for layer in (0, 1):
                self.scatter3.wait(layer)
                terms = (piece.third(sum2.at[layer], pos[a3]), recv3.at[1, layer], recv3.at[2, layer])
                for j in range(piece.lead3[0]):
                    g = terms[0][j] + terms[1][j].astype(F32) + terms[2][j].astype(F32)
                    g = g.astype(BF16).astype(F32)
                    if k < 2:
                        rows, cols = pl.ds(8 * j, 8), piece.columns()
                        w, m, v = adamw(
                            w_in[k][layer, j, :, cols].astype(F32), m_win[k][layer, rows, cols], v_win[k][layer, rows, cols], g
                        )
                        m_win[k][layer, rows, cols] = m
                        v_win[k][layer, rows, cols] = v
                        row = lax.broadcasted_iota(jnp.int32, w.shape, 0) + 8 * j
                        mine = (row >= 2 * pos[2]) & (row < 2 * pos[2] + 10)
                        self.buf[8][pos[2], layer, j] = jnp.where(mine, w, 0.0).astype(BF16)
                    else:
                        t = piece.chunk * TILES + j
                        w, m, v = adamw(w_in[k][layer, t].astype(F32), m_in[k][layer, t], v_in[k][layer, t], g)
                        new_m[k][layer, t] = m
                        new_v[k][layer, t] = v
                        new_w[k][layer, pos[0], pos[1], pos[2], t] = w.astype(BF16)
            self.gather3.start()

        def forward3(self):
            self.gather3.forward()

        def merge(self):
            piece = self.piece
            self.gather3.finish()
            if piece.weight < 2:
                windows, k = self.buf[8], piece.weight
                for layer in (0, 1):
                    for t in range(5):
                        parts = [windows[t - 1, layer, 1]] if t else []
                        parts += [windows[t, layer, 0]] if t < 4 else []
                        whole = parts[0] if len(parts) == 1 else (parts[0].astype(F32) + parts[1].astype(F32)).astype(BF16)
                        new_w[k][layer, pos[0], pos[1], t, :, piece.columns()] = whole
            self.gather2.start()

        def forward2(self):
            self.gather2.forward()

        def out1(self):
            self.gather2.finish()
            self.gather1.start()

        def forward1(self):
            self.gather1.forward()

        def done(self):
            self.gather1.finish()

    flows = [Flow(p, b) for p, b in zip(PIECES, bufs, strict=True)]
    groups = [flows[3 * c : 3 * c + 3] for c in range(CHUNKS)]

    for f in flows:
        f.load()
    state_loads = []
    for k in range(3):
        state_loads.append([load(ms[k], m_in[k]), load(vs[k], v_in[k])])
        own = weights[k].at[:, pos[0], pos[1], pl.ds(pos[2], 2)] if k < 2 else weights[k].at[:, pos[0], pos[1], pos[2]]
        state_loads[k].append(load(own, w_in[k]))
    pl.semaphore_wait(barrier, 6)

    def do(c, *names):
        for name in names:
            for f in groups[c]:
                getattr(f, name)()

    do(0, "far1", "near1")
    for k in range(3):
        for copy in state_loads[k]:
            copy.wait()
    for k in range(2):
        for win, data in ((m_win[k], m_in[k]), (v_win[k], v_in[k])):
            win[...] = jnp.zeros_like(win)
            for layer in (0, 1):
                for r in range(10):
                    win[layer, pl.ds(2 * pos[2] + r, 1), :] = data[r, pl.ds(layer, 1), :]
    do(0, "relay1")
    do(1, "far1")
    do(0, "sum1")
    do(1, "near1", "relay1")
    do(0, "relay2", "sum2", "relay3", "step", "forward3", "merge", "forward2")
    do(1, "sum1")
    do(0, "out1")
    do(1, "relay2", "sum2")
    do(0, "forward1")
    do(1, "relay3", "step", "forward3", "merge", "forward2", "out1", "forward1")

    for k in range(2):
        for win, out in ((m_win[k], new_m[k]), (v_win[k], new_v[k])):
            for layer in (0, 1):
                for r in range(10):
                    out[r, pl.ds(layer, 1), :] = win[layer, pl.ds(2 * pos[2] + r, 1), :]
    do(0, "done")
    do(1, "done")
    for copy in sent:
        copy.wait_send()


def solution(mesh):
    def step(*arrays):
        terms, weights, m, v = (arrays[i : i + 3] for i in (0, 3, 6, 9))
        shapes = ((2, 4, 4, 5, 8, 2048), (2, 4, 4, 5, 8, 2048), (2, 4, 4, 4, 4, 8, 640))
        terms = [t.reshape(s) for t, s in zip(terms, shapes, strict=True)]
        weights = [w.reshape(s) for w, s in zip(weights, shapes, strict=True)]

        def state_in(x):
            return x.transpose(1, 0, 2) if x.shape[1] == 10 else x.reshape(2, 4, 8, 640)

        m, v = [state_in(x) for x in m], [state_in(x) for x in v]
        state_shapes = [x.shape for x in m]
        outs = [(s, BF16) for s in shapes] + [(s, F32) for s in state_shapes] * 2
        scratch = [pltpu.VMEM(s, F32) for s in state_shapes] * 2
        scratch += [pltpu.VMEM((2, 2, 8, 2048), BF16)] * 2 + [pltpu.VMEM((2, 4, 8, 640), BF16)]
        scratch += [pltpu.VMEM((2, 16, 2048), F32)] * 4
        scratch += [pltpu.VMEM(s, d) for p in PIECES for s, d in p.scratch()]
        scratch += [pltpu.SemaphoreType.DMA((COPIES,)), pltpu.SemaphoreType.DMA((COPIES,)), pltpu.SemaphoreType.DMA((LOADS,))]
        new = pl.pallas_call(
            kernel,
            name="step",
            out_shape=[pltpu.VMEM(s, d) for s, d in outs],
            in_specs=[pl.BlockSpec(memory_space=pl.ANY)] * 12,
            out_specs=[pl.BlockSpec(memory_space=pltpu.VMEM)] * 9,
            scratch_shapes=scratch,
            compiler_params=pltpu.CompilerParams(collective_id=0, has_side_effects=True, vmem_limit_bytes=46 * 2**20),
        )(*terms, *weights, *m, *v)

        def state_out(x):
            return x.transpose(1, 0, 2) if x.shape[0] == 10 else x.reshape(2, 32, 640)

        whole = [w.reshape(s) for w, s in zip(new[:3], ((2, 640, 2048), (2, 640, 2048), (2, 2048, 640)), strict=True)]
        return (*whole, *(state_out(x) for x in new[3:]))

    all_of, cut = P(None, None, None), P(None, "dp", None)
    return jax.shard_map(
        step,
        mesh=mesh,
        in_specs=(P(("rep", "dp"), None, None, None),) * 3 + (all_of,) * 3 + (cut,) * 6,
        out_specs=(P("rep", None, None),) * 3 + (P("rep", "dp", None),) * 6,
        check_vma=False,
    )
```

```python
import jax
import jax.numpy as jnp
from jax import lax
from jax.experimental import pallas as pl
from jax.experimental.pallas import tpu as pltpu
from jax.sharding import PartitionSpec as P

STAGES = (
    *("far1", "near1", "relay1", "sum1", "relay2", "sum2", "relay3", "step"),
    *("forward3", "merge", "forward2", "out1", "rest1", "forward1"),
)
ORDER = (
    "abcabcabcdefeabcfefddabcihfieadgibcehhfagdlcgeibalklehbafgdc"
    "jihkfkgcjlebjaidhfebdhekdgchldjfgahbilgehdkjgcaifgdbljiefhjg"
    "kcjkcicbbjaaklfhgijkfleefkjddilkihggiljhkljkljkl"
)

MESH = pl.DeviceIdType.MESH
F32, BF16 = jnp.float32, jnp.bfloat16
CHUNKS = 4
COLS = 2048 // CHUNKS
TILES = 4 // CHUNKS


class Piece:
    def __init__(self, weight, chunk):
        self.weight, self.chunk = weight, chunk
        if weight < 2:
            self.axes = ((0, 1, 2), (1, 0, 2))[weight]
            self.lead1, self.lead2, self.lead3 = (4, 5), (5,), (2,)
            self.cols = COLS
        else:
            self.axes = ((2, 0, 1), (2, 1, 0))[chunk % 2]
            self.lead1, self.lead2, self.lead3 = (4, 4, TILES), (4, TILES), (TILES,)
            self.cols = 640

    def shape(self, lead, *front):
        return (*front, *lead, 8, self.cols)

    def scratch(self):
        one, two, three = self.lead1, self.lead2, self.lead3
        shapes = [
            (self.shape(one, 2, 2), BF16),
            (self.shape(one, 3, 2), BF16),
            (self.shape(two, 2, 2), F32),
            (self.shape(two, 2, 2), BF16),
            (self.shape(two, 3, 2), BF16),
            (self.shape(two, 2), F32),
            (self.shape(two, 2), BF16),
            (self.shape(three, 3, 2), BF16),
        ]
        if self.weight < 2:
            shapes.append((self.shape(three, 4, 2), BF16))
        return shapes

    def columns(self):
        return pl.ds(self.chunk * COLS, COLS)

    def first(self, ref, layer, p):
        if self.weight == 0:
            return ref.at[layer, p, :, :, :, self.columns()]
        if self.weight == 1:
            return ref.at[layer, :, p, :, :, self.columns()]
        return ref.at[layer, :, :, p, pl.ds(self.chunk * TILES, TILES)]

    def second(self, block, p):
        if self.weight == 2 and self.axes[1] == 1:
            return block.at[:, p]
        return block.at[p]

    def third(self, block, p):
        return block.at[pl.ds(p, 2)] if self.weight < 2 else block.at[p]

    def out2(self, ref, layer, p, pos):
        if self.weight == 0:
            return ref.at[layer, pos[0], p, :, :, self.columns()]
        if self.weight == 1:
            return ref.at[layer, p, pos[1], :, :, self.columns()]
        rows = pl.ds(self.chunk * TILES, TILES)
        if self.axes[1] == 0:
            return ref.at[layer, p, :, pos[2], rows]
        return ref.at[layer, :, p, pos[2], rows]

    def out3(self, ref, layer, p, pos):
        rows = pl.ds(self.chunk * TILES, TILES)
        if self.axes[2] == 1:
            return ref.at[layer, pos[0], p, pos[2], rows]
        return ref.at[layer, p, pos[1], pos[2], rows]


PIECES = [Piece(w, c) for c in range(CHUNKS) for w in range(3)]
COPIES = [12 * n for n in (3 * CHUNKS, 3 * CHUNKS, 2 * CHUNKS, CHUNKS)]
LOADS = 4 * len(PIECES) + 9


def add_into(lead, terms, outs):
    def body(index):
        total = terms[0][index].astype(F32)
        for t in terms[1:]:
            total = total + t[index].astype(F32)
        for o in outs:
            o[index] = total.astype(o.dtype)

    if len(lead) + (lead[-1] == 5) > 2:
        lax.fori_loop(0, lead[0], lambda i, c: (body(i), c)[1], 0)
    else:
        body(...)


def adamw(w, m, v, g):
    m = 0.9 * m + 0.1 * g
    v = 0.95 * v + 0.05 * g * g
    step = m * lax.rsqrt(v + 1e-8) + 0.1 * w
    return w - 0.02 * step, m, v


def kernel(*refs):
    refs = list(refs)

    def take(n):
        got, refs[:n] = refs[:n], []
        return got

    grads, weights, ms, vs = take(3), take(3), take(3), take(3)
    new_w, new_m, new_v = take(3), take(3), take(3)
    m_in, v_in, w_in = take(3), take(3), take(3)
    m_win, v_win = take(2), take(2)
    bufs = [take(len(p.scratch())) for p in PIECES]
    send_sems, recv_sems = take(4), take(4)
    (load_sem,) = take(1)

    me = lax.axis_index("dp")
    pos = (lax.div(me, 16), lax.rem(lax.div(me, 4), 4), lax.rem(me, 4))
    stride = (16, 4, 1)

    def at(axis, d):
        return lax.rem(pos[axis] + d, 4)

    def neighbour(axis, d):
        return me + (at(axis, d) - pos[axis]) * stride[axis]

    plus = [neighbour(a, 1) for a in range(3)]
    minus = [neighbour(a, 3) for a in range(3)]

    barrier = pltpu.get_barrier_semaphore()
    for other in (*plus, *minus):
        pl.semaphore_signal(barrier, inc=1, device_id={"dp": other}, device_id_type=MESH)

    sent, loads = [[], [], [], []], []

    def remote(src, dst, axis, forward, kind):
        i = len(sent[kind])
        copy = pltpu.make_async_remote_copy(
            src_ref=src,
            dst_ref=dst,
            send_sem=send_sems[kind].at[i],
            recv_sem=recv_sems[kind].at[i],
            device_id={"dp": (plus if forward else minus)[axis]},
            device_id_type=MESH,
        )
        sent[kind].append((src, dst))
        copy.start()
        return copy

    def wait_sent(kind):
        src, dst = sent[kind][0]

        def one(i, c):
            pltpu.make_async_remote_copy(
                src_ref=src,
                dst_ref=dst,
                send_sem=send_sems[kind].at[i],
                recv_sem=recv_sems[kind].at[i],
                device_id={"dp": plus[0]},
                device_id_type=MESH,
            ).wait_send()
            return c

        lax.fori_loop(0, len(sent[kind]), one, 0)

    def load(src, dst):
        copy = pltpu.make_async_copy(src, dst, load_sem.at[len(loads)])
        loads.append(copy)
        copy.start()
        return copy

    class Scatter:
        def __init__(self, kind, axis, recv, far, near, lead, relay_term):
            self.kind, self.axis, self.recv, self.far, self.near = kind, axis, recv, far, near
            self.lead, self.relay_term = lead, relay_term
            self.got = {}

        def send_far(self):
            for layer in (0, 1):
                self.got["far", layer] = remote(self.far(layer), self.recv.at[0, layer], self.axis, layer == 0, self.kind)

        def send_near(self):
            for layer in (1, 0):
                self.got["near", layer] = remote(self.near(layer), self.recv.at[1, layer], self.axis, layer == 1, self.kind)

        def relay(self):
            for layer in (0, 1):
                self.got["far", layer].wait_recv()
                here = self.recv.at[0, layer]
                add_into(self.lead, (here, self.relay_term(layer)), (here,))
                self.got["relay", layer] = remote(here, self.recv.at[2, layer], self.axis, layer == 0, self.kind)

        def wait(self, layer):
            self.got["near", layer].wait_recv()
            self.got["relay", layer].wait_recv()

    class Gather:
        def __init__(self, kind, axis, block):
            self.kind, self.axis, self.block = kind, axis, block
            self.got = {}

        def send(self, layer, p, forward, key):
            ref = self.block(layer, p)
            self.got[key] = remote(ref, ref, self.axis, forward, self.kind)

        def start(self):
            mine = pos[self.axis]
            self.send(0, mine, True, "from minus 0")
            self.send(1, mine, False, "from plus 1")

        def start_rest(self):
            mine = pos[self.axis]
            self.send(1, mine, True, "from minus 1")
            self.send(0, mine, False, "from plus 0")

        def forward(self):
            self.got["from minus 0"].wait_recv()
            self.send(0, at(self.axis, 3), True, "far 0")
            self.got["from plus 1"].wait_recv()
            self.send(1, at(self.axis, 1), False, "far 1")

        def finish(self):
            for key in ("from minus 1", "from plus 0", "far 0", "far 1"):
                self.got[key].wait_recv()

    class Flow:
        def __init__(self, piece, buf):
            self.piece, self.buf = piece, buf
            a1, a2, a3 = piece.axes
            last = 2 if piece.weight < 2 else 3
            g = grads[piece.weight]
            own1, recv1, sum1, send1, recv2, sum2, send2, recv3 = buf[:8]
            self.scatter1 = Scatter(
                0,
                a1,
                recv1,
                lambda layer: piece.first(g, layer, at(a1, 2)),
                lambda layer: piece.first(g, layer, at(a1, 1 if layer else 3)),
                piece.lead1,
                lambda layer: own1.at[layer, 1],
            )
            self.scatter2 = Scatter(
                1,
                a2,
                recv2,
                lambda layer: send1.at[layer, 0],
                lambda layer: send1.at[layer, 1],
                piece.lead2,
                lambda layer: sum1.at[layer, 1],
            )
            self.scatter3 = Scatter(
                last,
                a3,
                recv3,
                lambda layer: piece.third(send2.at[layer], at(a3, 2)),
                lambda layer: piece.third(send2.at[layer], at(a3, 1 if layer else 3)),
                piece.lead3,
                lambda layer: piece.third(sum2.at[layer], at(a3, 3 if layer else 1)),
            )
            w = new_w[piece.weight]
            if piece.weight < 2:
                windows = buf[8]
                self.gather3 = Gather(last, a3, lambda layer, p: windows.at[p, layer])
            else:
                self.gather3 = Gather(last, a3, lambda layer, p: piece.out3(w, layer, p, pos))
            self.gather2 = Gather(1, a2, lambda layer, p: piece.out2(w, layer, p, pos))
            self.gather1 = Gather(0, a1, lambda layer, p: piece.first(w, layer, p))

        def load(self):
            piece, own1 = self.piece, self.buf[0]
            a1, g = piece.axes[0], grads[piece.weight]
            self.loaded = [[None, None], [None, None]]
            for which in (1, 0):
                for layer in (0, 1):
                    p = at(a1, (3 if layer else 1) if which else 0)
                    self.loaded[layer][which] = load(piece.first(g, layer, p), own1.at[layer, which])

        def far1(self):
            self.scatter1.send_far()

        def near1(self):
            self.scatter1.send_near()

        def relay1(self):
            for layer in (0, 1):
                self.loaded[layer][1].wait()
            self.scatter1.relay()

        def sum1(self):
            piece = self.piece
            own1, recv1, sum1, send1 = self.buf[:4]
            a2 = piece.axes[1]
            for layer in (0, 1):
                self.loaded[layer][0].wait()
                self.scatter1.wait(layer)

            def reduce(layer, d, out):
                p = at(a2, d)
                terms = (own1.at[layer, 0], recv1.at[1, layer], recv1.at[2, layer])
                add_into(piece.lead2, [piece.second(t, p) for t in terms], (out,))

            for layer in (0, 1):
                reduce(layer, 2, send1.at[layer, 0])
            self.scatter2.send_far()
            for layer in (1, 0):
                reduce(layer, 1 if layer else 3, send1.at[layer, 1])
            self.scatter2.send_near()
            for layer in (0, 1):
                reduce(layer, 3 if layer else 1, sum1.at[layer, 1])
            for layer in (0, 1):
                reduce(layer, 0, sum1.at[layer, 0])

        def relay2(self):
            self.scatter2.relay()

        def sum2(self):
            sum1, _, recv2, sum2, send2 = self.buf[2:7]
            for layer in (0, 1):
                self.scatter2.wait(layer)
                terms = (sum1.at[layer, 0], recv2.at[1, layer], recv2.at[2, layer])
                add_into(self.piece.lead2, terms, (sum2.at[layer], send2.at[layer]))
            self.scatter3.send_far()
            self.scatter3.send_near()

        def relay3(self):
            self.scatter3.relay()

        def step(self):
            piece = self.piece
            sum2, recv3 = self.buf[5], self.buf[7]
            a3, k = piece.axes[2], piece.weight
            for layer in (0, 1):
                self.scatter3.wait(layer)
                terms = (piece.third(sum2.at[layer], pos[a3]), recv3.at[1, layer], recv3.at[2, layer])
                g = terms[0][...] + terms[1][...].astype(F32) + terms[2][...].astype(F32)
                g = g.astype(BF16).astype(F32)
                if k < 2:
                    cols = piece.columns()
                    w, m, v = w_in[k][layer, :, :, cols].astype(F32), m_win[k][layer, :, :, cols], v_win[k][layer, :, :, cols]
                    w, m, v = adamw(w, m, v, g)
                    m_win[k][layer, :, :, cols] = m
                    v_win[k][layer, :, :, cols] = v
                    row = lax.broadcasted_iota(jnp.int32, w.shape, 1) + 8 * lax.broadcasted_iota(jnp.int32, w.shape, 0)
                    mine = (row >= 2 * pos[2]) & (row < 2 * pos[2] + 10)
                    self.buf[8][pos[2], layer] = jnp.where(mine, w, 0.0).astype(BF16)
                else:
                    t = pl.ds(piece.chunk * TILES, TILES)
                    w, m, v = adamw(w_in[k][layer, t].astype(F32), m_in[k][layer, t], v_in[k][layer, t], g)
                    new_m[k][layer, t] = m
                    new_v[k][layer, t] = v
                    new_w[k][layer, pos[0], pos[1], pos[2], t] = w.astype(BF16)
            self.gather3.start()
            self.gather3.start_rest()

        def forward3(self):
            self.gather3.forward()

        def merge(self):
            piece = self.piece
            self.gather3.finish()
            if piece.weight < 2:
                windows, k = self.buf[8], piece.weight
                for layer in (0, 1):
                    out = new_w[k].at[layer, pos[0], pos[1], :, :, piece.columns()]
                    out[0] = windows[0, layer, 0]
                    both = windows[:3, layer, 1].astype(F32) + windows[1:, layer, 0].astype(F32)
                    out[1:4] = both.astype(BF16)
                    out[4] = windows[3, layer, 1]
            self.gather2.start()
            self.gather2.start_rest()

        def forward2(self):
            self.gather2.forward()

        def out1(self):
            self.gather2.finish()
            self.gather1.start()

        def rest1(self):
            self.gather1.start_rest()

        def forward1(self):
            self.gather1.forward()

        def done(self):
            self.gather1.finish()

    flows = [Flow(p, b) for p, b in zip(PIECES, bufs, strict=True)]
    for f in flows:
        f.load()
    state_loads = []
    for k in range(3):
        state_loads.append([load(ms[k], m_in[k]), load(vs[k], v_in[k])])
        own = weights[k].at[:, pos[0], pos[1], pl.ds(pos[2], 2)] if k < 2 else weights[k].at[:, pos[0], pos[1], pos[2]]
        state_loads[k].append(load(own, w_in[k]))
    pl.semaphore_wait(barrier, 6)

    def state_windows():
        for k in range(3):
            for copy in state_loads[k]:
                copy.wait()
        for k in range(2):
            for win in (m_win[k], v_win[k]):
                win[...] = jnp.zeros_like(win)

        def row(r, c):
            tile, at_row = lax.div(2 * pos[2] + r, 8), pl.ds(lax.rem(2 * pos[2] + r, 8), 1)
            for k in range(2):
                for win, data in ((m_win[k], m_in[k]), (v_win[k], v_in[k])):
                    for layer in (0, 1):
                        win[layer, tile, at_row, :] = data[r, pl.ds(layer, 1), :]
            return c

        lax.fori_loop(0, 10, row, 0)

    stage = [0] * len(flows)
    placed = False
    for letter in ORDER:
        i = ord(letter) - ord("a")
        if stage[i] == 2 and not placed:
            state_windows()
            placed = True
        getattr(flows[i], STAGES[stage[i]])()
        stage[i] += 1

    def row_out(r, c):
        tile, at_row = lax.div(2 * pos[2] + r, 8), pl.ds(lax.rem(2 * pos[2] + r, 8), 1)
        for k in range(2):
            for win, out in ((m_win[k], new_m[k]), (v_win[k], new_v[k])):
                for layer in (0, 1):
                    out[r, pl.ds(layer, 1), :] = win[layer, tile, at_row, :]
        return c

    lax.fori_loop(0, 10, row_out, 0)
    for f in flows:
        f.done()
    for kind in range(4):
        wait_sent(kind)


def solution(mesh):
    def step(*arrays):
        terms, weights, m, v = (arrays[i : i + 3] for i in (0, 3, 6, 9))
        shapes = ((2, 4, 4, 5, 8, 2048), (2, 4, 4, 5, 8, 2048), (2, 4, 4, 4, 4, 8, 640))
        terms = [t.reshape(s) for t, s in zip(terms, shapes, strict=True)]
        weights = [w.reshape(s) for w, s in zip(weights, shapes, strict=True)]

        def state_in(x):
            return x.transpose(1, 0, 2) if x.shape[1] == 10 else x.reshape(2, 4, 8, 640)

        m, v = [state_in(x) for x in m], [state_in(x) for x in v]
        state_shapes = [x.shape for x in m]
        outs = [(s, BF16) for s in shapes] + [(s, F32) for s in state_shapes] * 2
        scratch = [pltpu.VMEM(s, F32) for s in state_shapes] * 2
        scratch += [pltpu.VMEM((2, 2, 8, 2048), BF16)] * 2 + [pltpu.VMEM((2, 4, 8, 640), BF16)]
        scratch += [pltpu.VMEM((2, 2, 8, 2048), F32)] * 4
        scratch += [pltpu.VMEM(s, d) for p in PIECES for s, d in p.scratch()]
        scratch += [pltpu.SemaphoreType.DMA((n,)) for n in (*COPIES, *COPIES, LOADS)]
        new = pl.pallas_call(
            kernel,
            name="step",
            out_shape=[pltpu.VMEM(s, d) for s, d in outs],
            in_specs=[pl.BlockSpec(memory_space=pl.ANY)] * 12,
            out_specs=[pl.BlockSpec(memory_space=pltpu.VMEM)] * 9,
            scratch_shapes=scratch,
            compiler_params=pltpu.CompilerParams(collective_id=0, has_side_effects=True, vmem_limit_bytes=46 * 2**20),
        )(*terms, *weights, *m, *v)

        def put(*refs):
            sems = refs[18]
            copies = [pltpu.make_async_copy(refs[i], refs[9 + i], sems.at[i]) for i in range(9)]
            for copy in copies:
                copy.start()
            for copy in copies:
                copy.wait()

        new = pl.pallas_call(
            put,
            name="put",
            out_shape=[jax.ShapeDtypeStruct(s, d) for s, d in outs],
            in_specs=[pl.BlockSpec(memory_space=pltpu.VMEM)] * 9,
            out_specs=[pl.BlockSpec(memory_space=pl.ANY)] * 9,
            scratch_shapes=[pltpu.SemaphoreType.DMA((9,))],
            compiler_params=pltpu.CompilerParams(vmem_limit_bytes=2**20),
        )(*(pltpu.with_memory_space_constraint(x, pltpu.VMEM) for x in new))

        def state_out(x):
            return x.transpose(1, 0, 2) if x.shape[0] == 10 else x.reshape(2, 32, 640)

        whole = [w.reshape(s) for w, s in zip(new[:3], ((2, 640, 2048), (2, 640, 2048), (2, 2048, 640)), strict=True)]
        return (*whole, *(state_out(x) for x in new[3:]))

    all_of, cut = P(None, None, None), P(None, "dp", None)
    return jax.shard_map(
        step,
        mesh=mesh,
        in_specs=(P(("rep", "dp"), None, None, None),) * 3 + (all_of,) * 3 + (cut,) * 6,
        out_specs=(P("rep", None, None),) * 3 + (P("rep", "dp", None),) * 6,
        check_vma=False,
    )
```

```python
import jax
import jax.numpy as jnp
from jax import lax
from jax.experimental import pallas as pl
from jax.experimental.pallas import tpu as pltpu
from jax.sharding import PartitionSpec as P

STAGES = (
    *("far1", "near1", "relay1", "sum1", "relay2", "sum2", "relay3", "step"),
    *("forward3", "merge", "forward2", "out1", "rest1", "forward1"),
)
ORDER = (
    "abcabcabcdefeabcfefddabcihfieadgibcehhfagdlcgeibalklehbafgdc",
    "jihkfkgcjlebjaidhfebdhekdgchldjfgahbilgehdkjgcaifgdbljiefhjg",
    "kcjkcicbbjaaklfhgijkfleefkjddilkihggiljhkljkljkl",
)

MESH = pl.DeviceIdType.MESH
F32, BF16 = jnp.float32, jnp.bfloat16
CHUNKS = 4
COLS = 2048 // CHUNKS
TILES = 4 // CHUNKS


class Piece:
    def __init__(self, weight, chunk):
        self.weight, self.chunk = weight, chunk
        if weight < 2:
            self.axes = ((0, 1, 2), (1, 0, 2))[weight]
            self.lead1, self.lead2, self.lead3 = (4, 5), (5,), (2,)
            self.cols = COLS
        else:
            self.axes = ((2, 0, 1), (2, 1, 0))[chunk % 2]
            self.lead1, self.lead2, self.lead3 = (4, 4, TILES), (4, TILES), (TILES,)
            self.cols = 640

    def shape(self, lead, *front):
        return (*front, *lead, 8, self.cols)

    def scratch(self):
        one, two, three = self.lead1, self.lead2, self.lead3
        shapes = [
            (self.shape(one, 2, 2), BF16),
            (self.shape(one, 3, 2), BF16),
            (self.shape(two, 2, 2), F32),
            (self.shape(two, 2, 2), BF16),
            (self.shape(two, 3, 2), BF16),
            (self.shape(two, 2), F32),
            (self.shape(two, 2), BF16),
            (self.shape(three, 3, 2), BF16),
        ]
        if self.weight < 2:
            shapes.append((self.shape(three, 4, 2), BF16))
        return shapes

    def columns(self):
        return pl.ds(self.chunk * COLS, COLS)

    def first(self, ref, layer, p):
        if self.weight == 0:
            return ref.at[layer, p, :, :, :, self.columns()]
        if self.weight == 1:
            return ref.at[layer, :, p, :, :, self.columns()]
        return ref.at[layer, :, :, p, pl.ds(self.chunk * TILES, TILES)]

    def second(self, block, p):
        if self.weight == 2 and self.axes[1] == 1:
            return block.at[:, p]
        return block.at[p]

    def third(self, block, p):
        return block.at[pl.ds(p, 2)] if self.weight < 2 else block.at[p]

    def out2(self, ref, layer, p, pos):
        if self.weight == 0:
            return ref.at[layer, pos[0], p, :, :, self.columns()]
        if self.weight == 1:
            return ref.at[layer, p, pos[1], :, :, self.columns()]
        rows = pl.ds(self.chunk * TILES, TILES)
        if self.axes[1] == 0:
            return ref.at[layer, p, :, pos[2], rows]
        return ref.at[layer, :, p, pos[2], rows]

    def out3(self, ref, layer, p, pos):
        rows = pl.ds(self.chunk * TILES, TILES)
        if self.axes[2] == 1:
            return ref.at[layer, pos[0], p, pos[2], rows]
        return ref.at[layer, p, pos[1], pos[2], rows]


PIECES = [Piece(w, c) for c in range(CHUNKS) for w in range(3)]
MOVES = 6 * len(PIECES)
LOADS = 2 * len(PIECES) + 9


def add_into(lead, terms, outs):
    def body(index):
        total = terms[0][index].astype(F32)
        for t in terms[1:]:
            total = total + t[index].astype(F32)
        for o in outs:
            o[index] = total.astype(o.dtype)

    if len(lead) + (lead[-1] == 5) > 2:
        lax.fori_loop(0, lead[0], lambda i, c: (body(i), c)[1], 0)
    else:
        body(...)


def adamw(w, m, v, g):
    m = 0.9 * m + 0.1 * g
    v = 0.95 * v + 0.05 * g * g
    step = m * lax.rsqrt(v + 1e-8) + 0.1 * w
    return w - 0.02 * step, m, v


def kernel(*refs):
    refs = list(refs)

    def take(n):
        got, refs[:n] = refs[:n], []
        return got

    grads, weights, ms, vs = take(3), take(3), take(3), take(3)
    new_w, new_m, new_v = take(3), take(3), take(3)
    m_in, v_in, w_in = take(3), take(3), take(3)
    m_win, v_win = take(2), take(2)
    bufs = [take(len(p.scratch())) for p in PIECES]
    send_sem, recv_sem, load_sem = take(3)

    me = lax.axis_index("dp")
    pos = (lax.div(me, 16), lax.rem(lax.div(me, 4), 4), lax.rem(me, 4))
    stride = (16, 4, 1)

    def at(axis, d):
        return lax.rem(pos[axis] + d, 4)

    def neighbour(axis, d):
        return me + (at(axis, d) - pos[axis]) * stride[axis]

    plus = [neighbour(a, 1) for a in range(3)]
    minus = [neighbour(a, 3) for a in range(3)]

    barrier = pltpu.get_barrier_semaphore()
    for other in (*plus, *minus):
        pl.semaphore_signal(barrier, inc=1, device_id={"dp": other}, device_id_type=MESH)

    def wait(sem, like):
        pltpu.make_async_copy(like, like, sem).wait()

    def load(src, dst, sem):
        pltpu.make_async_copy(src, dst, sem).start()

    class Move:
        made = 0

        def __init__(self, axis, recv):
            self.axis, self.recv, self.index = axis, recv, Move.made
            Move.made += 1

        def remote(self, src, dst, forward, first):
            pltpu.make_async_remote_copy(
                src_ref=src,
                dst_ref=dst,
                send_sem=send_sem.at[self.index],
                recv_sem=recv_sem.at[2 * self.index + (0 if first else 1)],
                device_id={"dp": (plus if forward else minus)[self.axis]},
                device_id_type=MESH,
            ).start()

        def wait_first(self):
            wait(recv_sem.at[2 * self.index], self.recv.at[0])

        def wait_rest(self):
            wait(recv_sem.at[2 * self.index + 1], self.recv.at[pl.ds(1, 2)])

        def wait_sent(self):
            wait(send_sem.at[self.index], self.recv)

    class Scatter(Move):
        def __init__(self, axis, recv, far, near, lead, relay_term):
            super().__init__(axis, recv)
            self.far, self.near, self.lead, self.relay_term = far, near, lead, relay_term

        def send_far(self):
            for layer in (0, 1):
                self.remote(self.far(layer), self.recv.at[0, layer], layer == 0, True)

        def send_near(self):
            for layer in (1, 0):
                self.remote(self.near(layer), self.recv.at[1, layer], layer == 1, False)

        def relay(self):
            self.wait_first()
            for layer in (0, 1):
                here = self.recv.at[0, layer]
                add_into(self.lead, (here, self.relay_term(layer)), (here,))
                self.remote(here, self.recv.at[2, layer], layer == 0, False)

    class Gather(Move):
        def __init__(self, axis, recv, block):
            super().__init__(axis, recv)
            self.block = block

        def send(self, layer, p, forward, first):
            ref = self.block(layer, p)
            self.remote(ref, ref, forward, first)

        def start(self):
            mine = pos[self.axis]
            self.send(0, mine, True, True)
            self.send(1, mine, False, True)

        def start_rest(self):
            mine = pos[self.axis]
            self.send(1, mine, True, False)
            self.send(0, mine, False, False)

        def forward(self):
            self.wait_first()
            self.send(0, at(self.axis, 3), True, False)
            self.send(1, at(self.axis, 1), False, False)

    class Flow:
        def __init__(self, piece, buf):
            self.piece, self.buf = piece, buf
            a1, a2, a3 = piece.axes
            g = grads[piece.weight]
            own1, recv1, sum1, send1, recv2, sum2, send2, recv3 = buf[:8]
            self.scatter1 = Scatter(
                a1,
                recv1,
                lambda layer: piece.first(g, layer, at(a1, 2)),
                lambda layer: piece.first(g, layer, at(a1, 1 if layer else 3)),
                piece.lead1,
                lambda layer: own1.at[layer, 1],
            )
            self.scatter2 = Scatter(
                a2,
                recv2,
                lambda layer: send1.at[layer, 0],
                lambda layer: send1.at[layer, 1],
                piece.lead2,
                lambda layer: sum1.at[layer, 1],
            )
            self.scatter3 = Scatter(
                a3,
                recv3,
                lambda layer: piece.third(send2.at[layer], at(a3, 2)),
                lambda layer: piece.third(send2.at[layer], at(a3, 1 if layer else 3)),
                piece.lead3,
                lambda layer: piece.third(sum2.at[layer], at(a3, 3 if layer else 1)),
            )
            w = new_w[piece.weight]
            if piece.weight < 2:
                windows = buf[8]
                self.gather3 = Gather(a3, recv3, lambda layer, p: windows.at[p, layer])
            else:
                self.gather3 = Gather(a3, recv3, lambda layer, p: piece.out3(w, layer, p, pos))
            self.gather2 = Gather(a2, recv2, lambda layer, p: piece.out2(w, layer, p, pos))
            self.gather1 = Gather(a1, recv1, lambda layer, p: piece.first(w, layer, p))

            self.moves = (self.scatter1, self.scatter2, self.scatter3, self.gather3, self.gather2, self.gather1)

        def load(self, index):
            piece, own1 = self.piece, self.buf[0]
            a1, g = piece.axes[0], grads[piece.weight]
            self.loaded = [load_sem.at[2 * index], load_sem.at[2 * index + 1]]
            for which in (1, 0):
                for layer in (0, 1):
                    p = at(a1, (3 if layer else 1) if which else 0)
                    load(piece.first(g, layer, p), own1.at[layer, which], self.loaded[which])

        def far1(self):
            self.scatter1.send_far()

        def near1(self):
            self.scatter1.send_near()

        def relay1(self):
            wait(self.loaded[1], self.buf[0].at[:, 1])
            self.scatter1.relay()

        def sum1(self):
            piece = self.piece
            own1, recv1, sum1, send1 = self.buf[:4]
            a2 = piece.axes[1]
            wait(self.loaded[0], own1.at[:, 0])
            self.scatter1.wait_rest()

            def reduce(layer, d, out):
                p = at(a2, d)
                terms = (own1.at[layer, 0], recv1.at[1, layer], recv1.at[2, layer])
                add_into(piece.lead2, [piece.second(t, p) for t in terms], (out,))

            for layer in (0, 1):
                reduce(layer, 2, send1.at[layer, 0])
            self.scatter2.send_far()
            for layer in (1, 0):
                reduce(layer, 1 if layer else 3, send1.at[layer, 1])
            self.scatter2.send_near()
            for layer in (0, 1):
                reduce(layer, 3 if layer else 1, sum1.at[layer, 1])
            for layer in (0, 1):
                reduce(layer, 0, sum1.at[layer, 0])

        def relay2(self):
            self.scatter2.relay()

        def sum2(self):
            sum1, _, recv2, sum2, send2 = self.buf[2:7]
            self.scatter2.wait_rest()
            for layer in (0, 1):
                terms = (sum1.at[layer, 0], recv2.at[1, layer], recv2.at[2, layer])
                add_into(self.piece.lead2, terms, (sum2.at[layer], send2.at[layer]))
            self.scatter3.send_far()
            self.scatter3.send_near()

        def relay3(self):
            self.scatter3.relay()

        def step(self):
            piece = self.piece
            sum2, recv3 = self.buf[5], self.buf[7]
            a3, k = piece.axes[2], piece.weight
            self.scatter3.wait_rest()
            for layer in (0, 1):
                terms = (piece.third(sum2.at[layer], pos[a3]), recv3.at[1, layer], recv3.at[2, layer])
                g = terms[0][...] + terms[1][...].astype(F32) + terms[2][...].astype(F32)
                g = g.astype(BF16).astype(F32)
                if k < 2:
                    cols = piece.columns()
                    w, m, v = w_in[k][layer, :, :, cols].astype(F32), m_win[k][layer, :, :, cols], v_win[k][layer, :, :, cols]
                    w, m, v = adamw(w, m, v, g)
                    m_win[k][layer, :, :, cols] = m
                    v_win[k][layer, :, :, cols] = v
                    row = lax.broadcasted_iota(jnp.int32, w.shape, 1) + 8 * lax.broadcasted_iota(jnp.int32, w.shape, 0)
                    mine = (row >= 2 * pos[2]) & (row < 2 * pos[2] + 10)
                    self.buf[8][pos[2], layer] = jnp.where(mine, w, 0.0).astype(BF16)
                else:
                    t = pl.ds(piece.chunk * TILES, TILES)
                    w, m, v = adamw(w_in[k][layer, t].astype(F32), m_in[k][layer, t], v_in[k][layer, t], g)
                    new_m[k][layer, t] = m
                    new_v[k][layer, t] = v
                    new_w[k][layer, pos[0], pos[1], pos[2], t] = w.astype(BF16)
            self.gather3.start()
            self.gather3.start_rest()

        def forward3(self):
            self.gather3.forward()

        def merge(self):
            piece = self.piece
            self.gather3.wait_rest()
            if piece.weight < 2:
                windows, k = self.buf[8], piece.weight
                for layer in (0, 1):
                    out = new_w[k].at[layer, pos[0], pos[1], :, :, piece.columns()]
                    out[0] = windows[0, layer, 0]
                    both = windows[:3, layer, 1].astype(F32) + windows[1:, layer, 0].astype(F32)
                    out[1:4] = both.astype(BF16)
                    out[4] = windows[3, layer, 1]
            self.gather2.start()
            self.gather2.start_rest()

        def forward2(self):
            self.gather2.forward()

        def out1(self):
            self.gather2.wait_rest()
            self.gather1.start()

        def rest1(self):
            self.gather1.start_rest()

        def forward1(self):
            self.gather1.forward()

        def done(self):
            self.gather1.wait_rest()

    flows = [Flow(p, b) for p, b in zip(PIECES, bufs, strict=True)]
    for i, f in enumerate(flows):
        f.load(i)
    state = []
    for k in range(3):
        own = weights[k].at[:, pos[0], pos[1], pl.ds(pos[2], 2)] if k < 2 else weights[k].at[:, pos[0], pos[1], pos[2]]
        state += [(ms[k], m_in[k]), (vs[k], v_in[k]), (own, w_in[k])]
    for i, (src, dst) in enumerate(state):
        load(src, dst, load_sem.at[2 * len(flows) + i])
    pl.semaphore_wait(barrier, 6)

    def state_windows():
        for i, (_, dst) in enumerate(state):
            wait(load_sem.at[2 * len(flows) + i], dst)
        for k in range(2):
            for win in (m_win[k], v_win[k]):
                win[...] = jnp.zeros_like(win)

        def row(r, c):
            tile, at_row = lax.div(2 * pos[2] + r, 8), pl.ds(lax.rem(2 * pos[2] + r, 8), 1)
            for k in range(2):
                for win, data in ((m_win[k], m_in[k]), (v_win[k], v_in[k])):
                    for layer in (0, 1):
                        win[layer, tile, at_row, :] = data[r, pl.ds(layer, 1), :]
            return c

        lax.fori_loop(0, 10, row, 0)

    stage = [0] * len(flows)
    placed = False
    for letter in "".join(ORDER):
        i = ord(letter) - ord("a")
        if stage[i] == 2 and not placed:
            state_windows()
            placed = True
        getattr(flows[i], STAGES[stage[i]])()
        stage[i] += 1

    def row_out(r, c):
        tile, at_row = lax.div(2 * pos[2] + r, 8), pl.ds(lax.rem(2 * pos[2] + r, 8), 1)
        for k in range(2):
            for win, out in ((m_win[k], new_m[k]), (v_win[k], new_v[k])):
                for layer in (0, 1):
                    out[r, pl.ds(layer, 1), :] = win[layer, tile, at_row, :]
        return c

    lax.fori_loop(0, 10, row_out, 0)
    for f in flows:
        f.done()
    for f in flows:
        for move in f.moves:
            move.wait_sent()


def solution(mesh):
    def step(*arrays):
        terms, weights, m, v = (arrays[i : i + 3] for i in (0, 3, 6, 9))
        shapes = ((2, 4, 4, 5, 8, 2048), (2, 4, 4, 5, 8, 2048), (2, 4, 4, 4, 4, 8, 640))
        terms = [t.reshape(s) for t, s in zip(terms, shapes, strict=True)]
        weights = [w.reshape(s) for w, s in zip(weights, shapes, strict=True)]

        def state_in(x):
            return x.transpose(1, 0, 2) if x.shape[1] == 10 else x.reshape(2, 4, 8, 640)

        m, v = [state_in(x) for x in m], [state_in(x) for x in v]
        state_shapes = [x.shape for x in m]
        outs = [(s, BF16) for s in shapes] + [(s, F32) for s in state_shapes] * 2
        scratch = [pltpu.VMEM(s, F32) for s in state_shapes] * 2
        scratch += [pltpu.VMEM((2, 2, 8, 2048), BF16)] * 2 + [pltpu.VMEM((2, 4, 8, 640), BF16)]
        scratch += [pltpu.VMEM((2, 2, 8, 2048), F32)] * 4
        scratch += [pltpu.VMEM(s, d) for p in PIECES for s, d in p.scratch()]
        scratch += [pltpu.SemaphoreType.DMA((n,)) for n in (MOVES, 2 * MOVES, LOADS)]
        new = pl.pallas_call(
            kernel,
            name="step",
            out_shape=[pltpu.VMEM(s, d) for s, d in outs],
            in_specs=[pl.BlockSpec(memory_space=pl.ANY)] * 12,
            out_specs=[pl.BlockSpec(memory_space=pltpu.VMEM)] * 9,
            scratch_shapes=scratch,
            compiler_params=pltpu.CompilerParams(collective_id=0, has_side_effects=True, vmem_limit_bytes=46 * 2**20),
        )(*terms, *weights, *m, *v)

        def put(*refs):
            sems = refs[18]
            copies = [pltpu.make_async_copy(refs[i], refs[9 + i], sems.at[i]) for i in range(9)]
            for copy in copies:
                copy.start()
            for copy in copies:
                copy.wait()

        new = pl.pallas_call(
            put,
            name="put",
            out_shape=[jax.ShapeDtypeStruct(s, d) for s, d in outs],
            in_specs=[pl.BlockSpec(memory_space=pltpu.VMEM)] * 9,
            out_specs=[pl.BlockSpec(memory_space=pl.ANY)] * 9,
            scratch_shapes=[pltpu.SemaphoreType.DMA((9,))],
            compiler_params=pltpu.CompilerParams(vmem_limit_bytes=2**20),
        )(*(pltpu.with_memory_space_constraint(x, pltpu.VMEM) for x in new))

        def state_out(x):
            return x.transpose(1, 0, 2) if x.shape[0] == 10 else x.reshape(2, 32, 640)

        whole = [w.reshape(s) for w, s in zip(new[:3], ((2, 640, 2048), (2, 640, 2048), (2, 2048, 640)), strict=True)]
        return (*whole, *(state_out(x) for x in new[3:]))

    all_of, cut = P(None, None, None), P(None, "dp", None)
    return jax.shard_map(
        step,
        mesh=mesh,
        in_specs=(P(("rep", "dp"), None, None, None),) * 3 + (all_of,) * 3 + (cut,) * 6,
        out_specs=(P("rep", None, None),) * 3 + (P("rep", "dp", None),) * 6,
        check_vma=False,
    )
```

```python
import jax
import jax.numpy as jnp
from jax import lax
from jax.experimental import pallas as pl
from jax.experimental.pallas import tpu as pltpu
from jax.sharding import PartitionSpec as P

STAGES = (
    *("far1", "near1", "relay1", "sum1", "relay2", "sum2", "relay3", "step"),
    *("forward3", "merge", "forward2", "out1", "rest1", "forward1"),
)
ORDER = (
    "cadafcedbabbceffiebcadhegabgcdihaffjgcdheibkcladfhbgelfhckjg",
    "dkjcfabilgdhkjafbdgielckjbgahileahgecjkfdlbighkacliebaiklhdb",
    "bifgljkejchdeikcfahghjkliigjlldjikkhgjflfeekldjj",
)

MESH = pl.DeviceIdType.MESH
F32, BF16 = jnp.float32, jnp.bfloat16
CHUNKS = 4
COLS = 2048 // CHUNKS
EARLY = 1
TILES = 4 // CHUNKS


class Piece:
    def __init__(self, weight, chunk):
        self.weight, self.chunk = weight, chunk
        self.early = weight < 2 and chunk == EARLY
        if weight < 2:
            self.axes = ((0, 2, 1), (1, 2, 0))[weight] if self.early else ((0, 1, 2), (1, 0, 2))[weight]
            self.lead1, self.lead2, self.lead3 = (4, 5), (4, 2) if self.early else (5,), (2,)
            self.cols = COLS
        else:
            self.axes = ((2, 0, 1), (2, 1, 0))[chunk % 2]
            self.lead1, self.lead2, self.lead3 = (4, 4, TILES), (4, TILES), (TILES,)
            self.cols = 640

    def shape(self, lead, *front):
        return (*front, *lead, 8, self.cols)

    def scratch(self):
        one, two, three = self.lead1, self.lead2, self.lead3
        shapes = [
            (self.shape(one, 2, 2), BF16),
            (self.shape(one, 3, 2), BF16),
            (self.shape(two, 2, 2), F32),
            (self.shape(two, 2, 2), BF16),
            (self.shape(two, 3, 2), BF16),
            (self.shape(two, 2), F32),
            (self.shape(two, 2), BF16),
            (self.shape(three, 3, 2), BF16),
        ]
        if self.weight < 2:
            shapes.append((self.shape(two if self.early else three, 4, 2), BF16))
        return shapes

    def columns(self):
        return pl.ds(self.chunk * COLS, COLS)

    def first(self, ref, layer, p):
        if self.weight == 0:
            return ref.at[layer, p, :, :, :, self.columns()]
        if self.weight == 1:
            return ref.at[layer, :, p, :, :, self.columns()]
        return ref.at[layer, :, :, p, pl.ds(self.chunk * TILES, TILES)]

    def second(self, block, p):
        if self.early:
            return block.at[:, pl.ds(p, 2)]
        if self.weight == 2 and self.axes[1] == 1:
            return block.at[:, p]
        return block.at[p]

    def third(self, block, p):
        return block.at[p] if self.weight == 2 or self.early else block.at[pl.ds(p, 2)]

    def out2(self, ref, layer, p, pos):
        if self.weight == 0:
            return ref.at[layer, pos[0], p, :, :, self.columns()]
        if self.weight == 1:
            return ref.at[layer, p, pos[1], :, :, self.columns()]
        rows = pl.ds(self.chunk * TILES, TILES)
        if self.axes[1] == 0:
            return ref.at[layer, p, :, pos[2], rows]
        return ref.at[layer, :, p, pos[2], rows]

    def out3(self, ref, layer, p, pos):
        rows = pl.ds(self.chunk * TILES, TILES)
        if self.axes[2] == 1:
            return ref.at[layer, pos[0], p, pos[2], rows]
        return ref.at[layer, p, pos[1], pos[2], rows]


PIECES = [Piece(w, c) for c in range(CHUNKS) for w in range(3)]
MOVES = 3 * len(PIECES)
LOADS = 2 * CHUNKS + 4


def add_into(lead, terms, outs):
    def body(index):
        total = terms[0][index].astype(F32)
        for t in terms[1:]:
            total = total + t[index].astype(F32)
        for o in outs:
            o[index] = total.astype(o.dtype)

    if len(lead) > 2 or lead == (4, 5):
        lax.fori_loop(0, lead[0], lambda i, c: (body(i), c)[1], 0)
    else:
        body(...)


def adamw(w, m, v, g):
    m = 0.9 * m + 0.1 * g
    v = 0.95 * v + 0.05 * g * g
    step = m * lax.rsqrt(v + 1e-8) + 0.1 * w
    return w - 0.02 * step, m, v


def kernel(*refs):
    refs = list(refs)

    def take(n):
        got, refs[:n] = refs[:n], []
        return got

    grads, weights, ms, vs = take(3), take(3), take(3), take(3)
    new_w, new_m, new_v = take(3), take(3), take(3)
    m_in, v_in, w_in = take(3), take(3), take(3)
    m_win, v_win = take(2), take(2)
    bufs = [take(len(p.scratch())) for p in PIECES]
    send_sem, recv_sem, load_sem = take(3)

    me = lax.axis_index("dp")
    pos = (lax.div(me, 16), lax.rem(lax.div(me, 4), 4), lax.rem(me, 4))
    stride = (16, 4, 1)

    def at(axis, d):
        return lax.rem(pos[axis] + d, 4)

    def neighbour(axis, d):
        return me + (at(axis, d) - pos[axis]) * stride[axis]

    plus = [neighbour(a, 1) for a in range(3)]
    minus = [neighbour(a, 3) for a in range(3)]

    barrier = pltpu.get_barrier_semaphore()
    for other in (*plus, *minus):
        pl.semaphore_signal(barrier, inc=1, device_id={"dp": other}, device_id_type=MESH)

    def wait(sem, like):
        pltpu.make_async_copy(like, like, sem).wait()

    loaded = set()

    def load(src, dst, sem):
        pltpu.make_async_copy(src, dst, sem).start()

    class Move:
        def __init__(self, index, axis, recv):
            self.axis, self.recv, self.sems = axis, recv, (3 * index, 3 * index + self.rest)
            self.sent = send_sem.at[index]

        def remote(self, src, dst, forward, first):
            pltpu.make_async_remote_copy(
                src_ref=src,
                dst_ref=dst,
                send_sem=self.sent,
                recv_sem=recv_sem.at[self.sems[0 if first else 1]],
                device_id={"dp": (plus if forward else minus)[self.axis]},
                device_id_type=MESH,
            ).start()

        def wait_first(self):
            wait(recv_sem.at[self.sems[0]], self.recv.at[0])

        def wait_rest(self):
            wait(recv_sem.at[self.sems[1]], self.recv.at[pl.ds(1, 2)])

        def wait_sent(self):
            wait(self.sent, self.recv)

    class Scatter(Move):
        rest = 1

        def __init__(self, index, axis, recv, far, near, lead, relay_term):
            super().__init__(index, axis, recv)
            self.far, self.near, self.lead, self.relay_term = far, near, lead, relay_term

        def send_far(self):
            for layer in (0, 1):
                self.remote(self.far(layer), self.recv.at[0, layer], layer == 0, True)

        def send_near(self):
            for layer in (1, 0):
                self.remote(self.near(layer), self.recv.at[1, layer], layer == 1, False)

        def relay(self):
            self.wait_first()
            for layer in (0, 1):
                here = self.recv.at[0, layer]
                add_into(self.lead, (here, self.relay_term(layer)), (here,))
                self.remote(here, self.recv.at[2, layer], layer == 0, False)

    class Gather(Move):
        rest = 2

        def __init__(self, scatter, index, block):
            super().__init__(index, scatter.axis, scatter.recv)
            self.scatter, self.block = scatter, block

        def send(self, layer, p, forward, first):
            ref = self.block(layer, p)
            self.remote(ref, ref, forward, first)

        def start(self):
            self.scatter.wait_sent()
            mine = pos[self.axis]
            self.send(0, mine, True, True)
            self.send(1, mine, False, True)

        def start_rest(self):
            mine = pos[self.axis]
            self.send(1, mine, True, False)
            self.send(0, mine, False, False)

        def forward(self):
            self.wait_first()
            self.send(0, at(self.axis, 3), True, False)
            self.send(1, at(self.axis, 1), False, False)

    class Flow:
        def __init__(self, index, piece, buf):
            self.piece, self.buf = piece, buf
            a1, a2, a3 = piece.axes
            g = grads[piece.weight]
            own1, recv1, sum1, send1, recv2, sum2, send2, recv3 = buf[:8]
            self.scatter1 = Scatter(
                3 * index,
                a1,
                recv1,
                lambda layer: piece.first(g, layer, at(a1, 2)),
                lambda layer: piece.first(g, layer, at(a1, 1 if layer else 3)),
                piece.lead1,
                lambda layer: own1.at[layer, 1],
            )
            self.scatter2 = Scatter(
                3 * index + 1,
                a2,
                recv2,
                lambda layer: send1.at[layer, 0],
                lambda layer: send1.at[layer, 1],
                piece.lead2,
                lambda layer: sum1.at[layer, 1],
            )
            self.scatter3 = Scatter(
                3 * index + 2,
                a3,
                recv3,
                lambda layer: piece.third(send2.at[layer], at(a3, 2)),
                lambda layer: piece.third(send2.at[layer], at(a3, 1 if layer else 3)),
                piece.lead3,
                lambda layer: piece.third(sum2.at[layer], at(a3, 3 if layer else 1)),
            )
            w = new_w[piece.weight]
            if piece.weight < 2:
                windows = buf[8]
                if piece.early:
                    self.gather3 = Gather(self.scatter3, 3 * index + 2, lambda layer, p: windows.at[pos[2], layer, p])
                else:
                    self.gather3 = Gather(self.scatter3, 3 * index + 2, lambda layer, p: windows.at[p, layer])
            else:
                self.gather3 = Gather(self.scatter3, 3 * index + 2, lambda layer, p: piece.out3(w, layer, p, pos))
            if piece.early:
                self.gather2 = Gather(self.scatter2, 3 * index + 1, lambda layer, p: windows.at[p, layer])
            else:
                self.gather2 = Gather(self.scatter2, 3 * index + 1, lambda layer, p: piece.out2(w, layer, p, pos))
            self.gather1 = Gather(self.scatter1, 3 * index, lambda layer, p: piece.first(w, layer, p))

        def load(self):
            piece, own1 = self.piece, self.buf[0]
            a1, g = piece.axes[0], grads[piece.weight]
            for which in (1, 0):
                for layer in (0, 1):
                    p = at(a1, (3 if layer else 1) if which else 0)
                    load(piece.first(g, layer, p), own1.at[layer, which], load_sem.at[2 * piece.chunk + which])

        def wait_load(self, which):
            i = 2 * self.piece.chunk + which
            if i not in loaded:
                loaded.add(i)
                wait(load_sem.at[i], self.buf[1])

        def far1(self):
            self.scatter1.send_far()

        def near1(self):
            self.scatter1.send_near()

        def relay1(self):
            self.wait_load(1)
            self.scatter1.relay()

        def sum1(self):
            piece = self.piece
            own1, recv1, sum1, send1 = self.buf[:4]
            a2 = piece.axes[1]
            self.wait_load(0)
            self.scatter1.wait_rest()

            def reduce(layer, d, out):
                p = at(a2, d)
                terms = (own1.at[layer, 0], recv1.at[1, layer], recv1.at[2, layer])
                add_into(piece.lead2, [piece.second(t, p) for t in terms], (out,))

            for layer in (0, 1):
                reduce(layer, 2, send1.at[layer, 0])
            self.scatter2.send_far()
            for layer in (1, 0):
                reduce(layer, 1 if layer else 3, send1.at[layer, 1])
            self.scatter2.send_near()
            for layer in (0, 1):
                reduce(layer, 3 if layer else 1, sum1.at[layer, 1])
            for layer in (0, 1):
                reduce(layer, 0, sum1.at[layer, 0])

        def relay2(self):
            self.scatter2.relay()

        def sum2(self):
            sum1, _, recv2, sum2, send2 = self.buf[2:7]
            self.scatter2.wait_rest()
            for layer in (0, 1):
                terms = (sum1.at[layer, 0], recv2.at[1, layer], recv2.at[2, layer])
                add_into(self.piece.lead2, terms, (sum2.at[layer], send2.at[layer]))
            self.scatter3.send_far()
            self.scatter3.send_near()

        def relay3(self):
            self.scatter3.relay()

        def step(self):
            piece = self.piece
            sum2, recv3 = self.buf[5], self.buf[7]
            a3, k = piece.axes[2], piece.weight
            self.scatter3.wait_rest()
            for layer in (0, 1):
                terms = (piece.third(sum2.at[layer], pos[a3]), recv3.at[1, layer], recv3.at[2, layer])
                g = terms[0][...] + terms[1][...].astype(F32) + terms[2][...].astype(F32)
                g = g.astype(BF16).astype(F32)
                if k < 2:
                    cols = piece.columns()
                    w, m, v = w_in[k][layer, :, :, cols].astype(F32), m_win[k][layer, :, :, cols], v_win[k][layer, :, :, cols]
                    w, m, v = adamw(w, m, v, g)
                    m_win[k][layer, :, :, cols] = m
                    v_win[k][layer, :, :, cols] = v
                    row = lax.broadcasted_iota(jnp.int32, w.shape, 1) + 8 * lax.broadcasted_iota(jnp.int32, w.shape, 0)
                    mine = (row >= 2 * pos[2]) & (row < 2 * pos[2] + 10)
                    windows = self.gather3.block(layer, pos[a3])
                    windows[...] = jnp.where(mine, w, 0.0).astype(BF16)
                else:
                    t = pl.ds(piece.chunk * TILES, TILES)
                    w, m, v = adamw(w_in[k][layer, t].astype(F32), m_in[k][layer, t], v_in[k][layer, t], g)
                    new_m[k][layer, t] = m
                    new_v[k][layer, t] = v
                    new_w[k][layer, pos[0], pos[1], pos[2], t] = w.astype(BF16)
            self.gather3.start()
            self.gather3.start_rest()

        def forward3(self):
            self.gather3.forward()

        def merge(self):
            self.gather3.wait_rest()
            if self.piece.weight < 2 and not self.piece.early:
                self.join(lambda t: (pos[self.piece.axes[1]], t))
            self.gather2.start()
            self.gather2.start_rest()

        def join(self, tile):
            piece, windows = self.piece, self.buf[8]
            for layer in (0, 1):
                out = piece.first(new_w[piece.weight], layer, pos[piece.axes[0]])
                part = [windows.at[z, layer, :, j] if piece.early else windows.at[z, layer, j] for z in range(4) for j in (0, 1)]
                out[tile(0)] = part[0][...]
                for t in (1, 2, 3):
                    out[tile(t)] = (part[2 * t - 1][...].astype(F32) + part[2 * t][...].astype(F32)).astype(BF16)
                out[tile(4)] = part[7][...]

        def forward2(self):
            self.gather2.forward()

        def out1(self):
            self.gather2.wait_rest()
            if self.piece.early:
                self.join(lambda t: (slice(None), t))
            self.gather1.start()

        def rest1(self):
            self.gather1.start_rest()

        def forward1(self):
            self.gather1.forward()

        def done(self):
            self.gather1.wait_rest()

    flows = [Flow(i, p, b) for i, (p, b) in enumerate(zip(PIECES, bufs, strict=True))]
    for f in flows:
        f.load()
    state_sem = 2 * CHUNKS
    for k in range(3):
        own = weights[k].at[:, pos[0], pos[1], pl.ds(pos[2], 2)] if k < 2 else weights[k].at[:, pos[0], pos[1], pos[2]]
        load(own, w_in[k], load_sem.at[state_sem + 1 + k])
        load(ms[k], m_in[k], load_sem.at[state_sem])
        load(vs[k], v_in[k], load_sem.at[state_sem])
    pl.semaphore_wait(barrier, 6)

    def state_windows():
        wait(load_sem.at[state_sem], bufs[0][1])
        for k in range(3):
            wait(load_sem.at[state_sem + 1 + k], w_in[k])
        for k in range(2):
            for win in (m_win[k], v_win[k]):
                win[...] = jnp.zeros_like(win)

        def row(r, c):
            tile, at_row = lax.div(2 * pos[2] + r, 8), pl.ds(lax.rem(2 * pos[2] + r, 8), 1)
            for k in range(2):
                for win, data in ((m_win[k], m_in[k]), (v_win[k], v_in[k])):
                    for layer in (0, 1):
                        win[layer, tile, at_row, :] = data[r, pl.ds(layer, 1), :]
            return c

        lax.fori_loop(0, 10, row, 0)

    stage = [0] * len(flows)
    placed = False
    for letter in "".join(ORDER):
        i = ord(letter) - ord("a")
        if stage[i] == 2 and not placed:
            state_windows()
            placed = True
        getattr(flows[i], STAGES[stage[i]])()
        stage[i] += 1

    def row_out(r, c):
        tile, at_row = lax.div(2 * pos[2] + r, 8), pl.ds(lax.rem(2 * pos[2] + r, 8), 1)
        for k in range(2):
            for win, out in ((m_win[k], new_m[k]), (v_win[k], new_v[k])):
                for layer in (0, 1):
                    out[r, pl.ds(layer, 1), :] = win[layer, tile, at_row, :]
        return c

    lax.fori_loop(0, 10, row_out, 0)
    for f in flows:
        f.done()
    for f in flows:
        for gather in (f.gather3, f.gather2, f.gather1):
            gather.wait_sent()


def solution(mesh):
    def step(*arrays):
        terms, weights, m, v = (arrays[i : i + 3] for i in (0, 3, 6, 9))
        shapes = ((2, 4, 4, 5, 8, 2048), (2, 4, 4, 5, 8, 2048), (2, 4, 4, 4, 4, 8, 640))
        terms = [t.reshape(s) for t, s in zip(terms, shapes, strict=True)]
        weights = [w.reshape(s) for w, s in zip(weights, shapes, strict=True)]

        def state_in(x):
            return x.transpose(1, 0, 2) if x.shape[1] == 10 else x.reshape(2, 4, 8, 640)

        m, v = [state_in(x) for x in m], [state_in(x) for x in v]
        state_shapes = [x.shape for x in m]
        outs = [(s, BF16) for s in shapes] + [(s, F32) for s in state_shapes] * 2
        scratch = [pltpu.VMEM(s, F32) for s in state_shapes] * 2
        scratch += [pltpu.VMEM((2, 2, 8, 2048), BF16)] * 2 + [pltpu.VMEM((2, 4, 8, 640), BF16)]
        scratch += [pltpu.VMEM((2, 2, 8, 2048), F32)] * 4
        scratch += [pltpu.VMEM(s, d) for p in PIECES for s, d in p.scratch()]
        scratch += [pltpu.SemaphoreType.DMA((n,)) for n in (MOVES, 3 * MOVES, LOADS)]
        new = pl.pallas_call(
            kernel,
            name="step",
            out_shape=[pltpu.VMEM(s, d) for s, d in outs],
            in_specs=[pl.BlockSpec(memory_space=pl.ANY)] * 12,
            out_specs=[pl.BlockSpec(memory_space=pltpu.VMEM)] * 9,
            scratch_shapes=scratch,
            compiler_params=pltpu.CompilerParams(collective_id=0, has_side_effects=True, vmem_limit_bytes=46 * 2**20),
        )(*terms, *weights, *m, *v)

        def put(*refs):
            sems = refs[18]
            copies = [pltpu.make_async_copy(refs[i], refs[9 + i], sems.at[i]) for i in range(9)]
            for copy in copies:
                copy.start()
            for copy in copies:
                copy.wait()

        new = pl.pallas_call(
            put,
            name="put",
            out_shape=[jax.ShapeDtypeStruct(s, d) for s, d in outs],
            in_specs=[pl.BlockSpec(memory_space=pltpu.VMEM)] * 9,
            out_specs=[pl.BlockSpec(memory_space=pl.ANY)] * 9,
            scratch_shapes=[pltpu.SemaphoreType.DMA((9,))],
            compiler_params=pltpu.CompilerParams(vmem_limit_bytes=2**20),
        )(*(pltpu.with_memory_space_constraint(x, pltpu.VMEM) for x in new))

        def state_out(x):
            return x.transpose(1, 0, 2) if x.shape[0] == 10 else x.reshape(2, 32, 640)

        whole = [w.reshape(s) for w, s in zip(new[:3], ((2, 640, 2048), (2, 640, 2048), (2, 2048, 640)), strict=True)]
        return (*whole, *(state_out(x) for x in new[3:]))

    all_of, cut = P(None, None, None), P(None, "dp", None)
    return jax.shard_map(
        step,
        mesh=mesh,
        in_specs=(P(("rep", "dp"), None, None, None),) * 3 + (all_of,) * 3 + (cut,) * 6,
        out_specs=(P("rep", None, None),) * 3 + (P("rep", "dp", None),) * 6,
        check_vma=False,
    )
```

```python
import jax
import jax.numpy as jnp
from jax import lax
from jax.experimental import pallas as pl
from jax.experimental.pallas import tpu as pltpu
from jax.sharding import PartitionSpec as P

STAGES = (
    *("far1", "near1", "relay1", "sum1", "relay2", "sum2", "relay3", "step"),
    *("forward3", "merge", "forward2", "out1", "rest1", "forward1"),
)
ORDER = (
    "cadafcedbabbceffiebcadhegabgcdihaffjgcdheibkcladfhbgelfhckjg",
    "dkjcfabilgdhkjafbdgielckjbgahileahgecjkfdlbighkacliebaiklhdb",
    "bifgljkejchdeikcfahghjkliigjlldjikkhgjflfeekldjj",
)

MESH = pl.DeviceIdType.MESH
F32, BF16 = jnp.float32, jnp.bfloat16
CHUNKS = 4
COLS = 2048 // CHUNKS
EARLY = 1
TILES = 4 // CHUNKS


class Piece:
    def __init__(self, weight, chunk):
        self.weight, self.chunk = weight, chunk
        self.early = weight < 2 and chunk == EARLY
        if weight < 2:
            self.axes = ((0, 2, 1), (1, 2, 0))[weight] if self.early else ((0, 1, 2), (1, 0, 2))[weight]
            self.lead1, self.lead2, self.lead3 = (4, 5), (4, 2) if self.early else (5,), (2,)
            self.cols = COLS
        else:
            self.axes = ((2, 0, 1), (2, 1, 0))[chunk % 2]
            self.lead1, self.lead2, self.lead3 = (4, 4, TILES), (4, TILES), (TILES,)
            self.cols = 640

    def shape(self, lead, *front):
        return (*front, *lead, 8, self.cols)

    def scratch(self):
        one, two, three = self.lead1, self.lead2, self.lead3
        shapes = [
            (self.shape(one, 2, 2), BF16),
            (self.shape(one, 3, 2), BF16),
            (self.shape(two, 2, 2), F32),
            (self.shape(two, 2, 2), BF16),
            (self.shape(two, 3, 2), BF16),
            (self.shape(two, 2), F32),
            (self.shape(two, 2), BF16),
            (self.shape(three, 3, 2), BF16),
        ]
        if self.weight < 2:
            shapes.append((self.shape(two if self.early else three, 4, 2), BF16))
        return shapes

    def columns(self):
        return pl.ds(self.chunk * COLS, COLS)

    def first(self, ref, layer, p):
        if self.weight == 0:
            return ref.at[layer, p, :, :, :, self.columns()]
        if self.weight == 1:
            return ref.at[layer, :, p, :, :, self.columns()]
        return ref.at[layer, :, :, p, pl.ds(self.chunk * TILES, TILES)]

    def second(self, block, p):
        if self.early:
            return block.at[:, pl.ds(p, 2)]
        if self.weight == 2 and self.axes[1] == 1:
            return block.at[:, p]
        return block.at[p]

    def third(self, block, p):
        return block.at[p] if self.weight == 2 or self.early else block.at[pl.ds(p, 2)]

    def out2(self, ref, layer, p, pos):
        if self.weight == 0:
            return ref.at[layer, pos[0], p, :, :, self.columns()]
        if self.weight == 1:
            return ref.at[layer, p, pos[1], :, :, self.columns()]
        rows = pl.ds(self.chunk * TILES, TILES)
        if self.axes[1] == 0:
            return ref.at[layer, p, :, pos[2], rows]
        return ref.at[layer, :, p, pos[2], rows]

    def out3(self, ref, layer, p, pos):
        rows = pl.ds(self.chunk * TILES, TILES)
        if self.axes[2] == 1:
            return ref.at[layer, pos[0], p, pos[2], rows]
        return ref.at[layer, p, pos[1], pos[2], rows]


PIECES = [Piece(w, c) for c in range(CHUNKS) for w in range(3)]
LOADS = 2 * CHUNKS + 5

RECEIVES = ((0, 1), (2, 3), (4, 5), (4, 3), (2, 1), (0, 6))


def add_into(lead, terms, outs):
    def body(index):
        total = terms[0][index].astype(F32)
        for t in terms[1:]:
            total = total + t[index].astype(F32)
        for o in outs:
            o[index] = total.astype(o.dtype)

    if len(lead) > 2 or lead == (4, 5):
        lax.fori_loop(0, lead[0], lambda i, c: (body(i), c)[1], 0)
    else:
        body(...)


def adamw(w, m, v, g):
    m = 0.9 * m + 0.1 * g
    v = 0.95 * v + 0.05 * g * g
    step = m * lax.rsqrt(v + 1e-8) + 0.1 * w
    return w - 0.02 * step, m, v


def kernel(*refs):
    refs = list(refs)

    def take(n):
        got, refs[:n] = refs[:n], []
        return got

    grads, weights, ms, vs = take(3), take(3), take(3), take(3)
    new_w, new_m, new_v = take(3), take(3), take(3)
    m_in, v_in, w_in = take(3), take(3), take(3)
    m_win, v_win = take(2), take(2)
    ahead = take(3)
    bufs = [take(len(p.scratch())) for p in PIECES]
    send_sem, recv_sem, load_sem = take(3)

    me = lax.axis_index("dp")
    pos = (lax.div(me, 16), lax.rem(lax.div(me, 4), 4), lax.rem(me, 4))
    stride = (16, 4, 1)

    def at(axis, d):
        return lax.rem(pos[axis] + d, 4)

    def neighbour(axis, d):
        return me + (at(axis, d) - pos[axis]) * stride[axis]

    plus = [neighbour(a, 1) for a in range(3)]
    minus = [neighbour(a, 3) for a in range(3)]

    barrier = pltpu.get_barrier_semaphore()
    for other in (*plus, *minus):
        pl.semaphore_signal(barrier, inc=1, device_id={"dp": other}, device_id_type=MESH)

    def wait(sem, like):
        pltpu.make_async_copy(like, like, sem).wait()

    loaded = set()

    def load(src, dst, sem):
        pltpu.make_async_copy(src, dst, sem).start()

    class Move:
        def __init__(self, index, stage, axis, recv):
            self.axis, self.recv = axis, recv
            self.sent = send_sem.at[2 * index + stage % 2]
            self.sems = [7 * index + i for i in RECEIVES[stage]]

        def remote(self, src, dst, forward, first):
            pltpu.make_async_remote_copy(
                src_ref=src,
                dst_ref=dst,
                send_sem=self.sent,
                recv_sem=recv_sem.at[self.sems[0 if first else 1]],
                device_id={"dp": (plus if forward else minus)[self.axis]},
                device_id_type=MESH,
            ).start()

        def wait_first(self):
            wait(recv_sem.at[self.sems[0]], self.recv.at[0])

        def wait_rest(self):
            wait(recv_sem.at[self.sems[1]], self.recv.at[pl.ds(1, 2)])

        def wait_sent(self):
            wait(self.sent, self.recv)

    class Scatter(Move):
        def __init__(self, index, stage, axis, recv, far, near, lead, relay_term):
            super().__init__(index, stage, axis, recv)
            self.far, self.near, self.lead, self.relay_term = far, near, lead, relay_term

        def send_far(self):
            for layer in (0, 1):
                self.remote(self.far(layer), self.recv.at[0, layer], layer == 0, True)

        def send_near(self):
            for layer in (1, 0):
                self.remote(self.near(layer), self.recv.at[1, layer], layer == 1, False)

        def relay(self):
            self.wait_first()
            for layer in (0, 1):
                here = self.recv.at[0, layer]
                add_into(self.lead, (here, self.relay_term(layer)), (here,))
                self.remote(here, self.recv.at[2, layer], layer == 0, False)

    class Gather(Move):
        def __init__(self, index, stage, scatter, block):
            super().__init__(index, stage, scatter.axis, scatter.recv)
            self.block = block

        def send(self, layer, p, forward, first):
            ref = self.block(layer, p)
            self.remote(ref, ref, forward, first)

        def start(self):
            mine = pos[self.axis]
            self.send(0, mine, True, True)
            self.send(1, mine, False, True)

        def start_rest(self):
            mine = pos[self.axis]
            self.send(1, mine, True, False)
            self.send(0, mine, False, False)

        def forward(self):
            self.wait_first()
            self.send(0, at(self.axis, 3), True, False)
            self.send(1, at(self.axis, 1), False, False)

    class Flow:
        def __init__(self, index, piece, buf):
            self.piece, self.buf = piece, buf
            a1, a2, a3 = piece.axes
            g = grads[piece.weight]
            own1, recv1, sum1, send1, recv2, sum2, send2, recv3 = buf[:8]
            self.scatter1 = Scatter(
                index,
                0,
                a1,
                recv1,
                lambda layer: piece.first(g, layer, at(a1, 2)) if piece.chunk else ahead[piece.weight].at[layer],
                lambda layer: piece.first(g, layer, at(a1, 1 if layer else 3)),
                piece.lead1,
                lambda layer: own1.at[layer, 1],
            )
            self.scatter2 = Scatter(
                index,
                1,
                a2,
                recv2,
                lambda layer: send1.at[layer, 0],
                lambda layer: send1.at[layer, 1],
                piece.lead2,
                lambda layer: sum1.at[layer, 1],
            )
            self.scatter3 = Scatter(
                index,
                2,
                a3,
                recv3,
                lambda layer: piece.third(send2.at[layer], at(a3, 2)),
                lambda layer: piece.third(send2.at[layer], at(a3, 1 if layer else 3)),
                piece.lead3,
                lambda layer: piece.third(sum2.at[layer], at(a3, 3 if layer else 1)),
            )
            w = new_w[piece.weight]
            if piece.weight < 2:
                windows = buf[8]
                if piece.early:
                    self.gather3 = Gather(index, 3, self.scatter3, lambda layer, p: windows.at[pos[2], layer, p])
                else:
                    self.gather3 = Gather(index, 3, self.scatter3, lambda layer, p: windows.at[p, layer])
            else:
                self.gather3 = Gather(index, 3, self.scatter3, lambda layer, p: piece.out3(w, layer, p, pos))
            if piece.early:
                self.gather2 = Gather(index, 4, self.scatter2, lambda layer, p: windows.at[p, layer])
            else:
                self.gather2 = Gather(index, 4, self.scatter2, lambda layer, p: piece.out2(w, layer, p, pos))
            self.gather1 = Gather(index, 5, self.scatter1, lambda layer, p: piece.first(w, layer, p))

        def load(self):
            piece, own1 = self.piece, self.buf[0]
            a1, g = piece.axes[0], grads[piece.weight]
            for which in (1, 0):
                for layer in (0, 1):
                    p = at(a1, (3 if layer else 1) if which else 0)
                    load(piece.first(g, layer, p), own1.at[layer, which], load_sem.at[2 * piece.chunk + which])

        def wait_load(self, which):
            i = 2 * self.piece.chunk + which
            if i not in loaded:
                loaded.add(i)
                wait(load_sem.at[i], self.buf[1])

        def far1(self):
            self.scatter1.send_far()

        def near1(self):
            self.scatter1.send_near()

        def relay1(self):
            self.wait_load(1)
            self.scatter1.relay()

        def sum1(self):
            piece = self.piece
            own1, recv1, sum1, send1 = self.buf[:4]
            a2 = piece.axes[1]
            self.wait_load(0)
            self.scatter1.wait_rest()

            def reduce(layer, d, out):
                p = at(a2, d)
                terms = (own1.at[layer, 0], recv1.at[1, layer], recv1.at[2, layer])
                add_into(piece.lead2, [piece.second(t, p) for t in terms], (out,))

            for layer in (0, 1):
                reduce(layer, 2, send1.at[layer, 0])
            self.scatter2.send_far()
            for layer in (1, 0):
                reduce(layer, 1 if layer else 3, send1.at[layer, 1])
            self.scatter2.send_near()
            for layer in (0, 1):
                reduce(layer, 3 if layer else 1, sum1.at[layer, 1])
            for layer in (0, 1):
                reduce(layer, 0, sum1.at[layer, 0])

        def relay2(self):
            self.scatter2.relay()

        def sum2(self):
            sum1, _, recv2, sum2, send2 = self.buf[2:7]
            self.scatter2.wait_rest()
            for layer in (0, 1):
                terms = (sum1.at[layer, 0], recv2.at[1, layer], recv2.at[2, layer])
                add_into(self.piece.lead2, terms, (sum2.at[layer], send2.at[layer]))
            self.scatter1.wait_sent()
            self.scatter3.send_far()
            self.scatter3.send_near()

        def relay3(self):
            self.scatter3.relay()

        def step(self):
            piece = self.piece
            sum2, recv3 = self.buf[5], self.buf[7]
            a3, k = piece.axes[2], piece.weight
            self.scatter3.wait_rest()
            for layer in (0, 1):
                terms = (piece.third(sum2.at[layer], pos[a3]), recv3.at[1, layer], recv3.at[2, layer])
                g = terms[0][...] + terms[1][...].astype(F32) + terms[2][...].astype(F32)
                g = g.astype(BF16).astype(F32)
                if k < 2:
                    cols = piece.columns()
                    w, m, v = w_in[k][layer, :, :, cols].astype(F32), m_win[k][layer, :, :, cols], v_win[k][layer, :, :, cols]
                    w, m, v = adamw(w, m, v, g)
                    m_win[k][layer, :, :, cols] = m
                    v_win[k][layer, :, :, cols] = v
                    row = lax.broadcasted_iota(jnp.int32, w.shape, 1) + 8 * lax.broadcasted_iota(jnp.int32, w.shape, 0)
                    mine = (row >= 2 * pos[2]) & (row < 2 * pos[2] + 10)
                    windows = self.gather3.block(layer, pos[a3])
                    windows[...] = jnp.where(mine, w, 0.0).astype(BF16)
                else:
                    t = pl.ds(piece.chunk * TILES, TILES)
                    w, m, v = adamw(w_in[k][layer, t].astype(F32), m_in[k][layer, t], v_in[k][layer, t], g)
                    new_m[k][layer, t] = m
                    new_v[k][layer, t] = v
                    new_w[k][layer, pos[0], pos[1], pos[2], t] = w.astype(BF16)
            self.scatter2.wait_sent()
            self.gather3.start()
            self.gather3.start_rest()

        def forward3(self):
            self.gather3.forward()

        def merge(self):
            self.gather3.wait_rest()
            if self.piece.weight < 2 and not self.piece.early:
                self.join(lambda t: (pos[self.piece.axes[1]], t))
            self.scatter3.wait_sent()
            self.gather2.start()
            self.gather2.start_rest()

        def join(self, tile):
            piece, windows = self.piece, self.buf[8]
            for layer in (0, 1):
                out = piece.first(new_w[piece.weight], layer, pos[piece.axes[0]])
                part = [windows.at[z, layer, :, j] if piece.early else windows.at[z, layer, j] for z in range(4) for j in (0, 1)]
                out[tile(0)] = part[0][...]
                for t in (1, 2, 3):
                    out[tile(t)] = (part[2 * t - 1][...].astype(F32) + part[2 * t][...].astype(F32)).astype(BF16)
                out[tile(4)] = part[7][...]

        def forward2(self):
            self.gather2.forward()

        def out1(self):
            self.gather2.wait_rest()
            if self.piece.early:
                self.join(lambda t: (slice(None), t))
            self.gather3.wait_sent()
            self.gather1.start()

        def rest1(self):
            self.gather1.start_rest()

        def forward1(self):
            self.gather1.forward()

        def done(self):
            self.gather1.wait_rest()

    flows = [Flow(i, p, b) for i, (p, b) in enumerate(zip(PIECES, bufs, strict=True))]
    for f, dst in zip(flows, ahead, strict=False):
        for layer in (0, 1):
            load(f.piece.first(grads[f.piece.weight], layer, at(f.piece.axes[0], 2)), dst.at[layer], load_sem.at[LOADS - 1])
    for f in flows:
        f.load()
    state_sem = 2 * CHUNKS
    for k in range(3):
        own = weights[k].at[:, pos[0], pos[1], pl.ds(pos[2], 2)] if k < 2 else weights[k].at[:, pos[0], pos[1], pos[2]]
        load(own, w_in[k], load_sem.at[state_sem + 1 + k])
        load(ms[k], m_in[k], load_sem.at[state_sem])
        load(vs[k], v_in[k], load_sem.at[state_sem])
    wait(load_sem.at[LOADS - 1], bufs[0][1])
    pl.semaphore_wait(barrier, 6)

    def state_windows():
        wait(load_sem.at[state_sem], bufs[0][1])
        for k in range(3):
            wait(load_sem.at[state_sem + 1 + k], w_in[k])
        for k in range(2):
            for win in (m_win[k], v_win[k]):
                win[...] = jnp.zeros_like(win)

        def row(r, c):
            tile, at_row = lax.div(2 * pos[2] + r, 8), pl.ds(lax.rem(2 * pos[2] + r, 8), 1)
            for k in range(2):
                for win, data in ((m_win[k], m_in[k]), (v_win[k], v_in[k])):
                    for layer in (0, 1):
                        win[layer, tile, at_row, :] = data[r, pl.ds(layer, 1), :]
            return c

        lax.fori_loop(0, 10, row, 0)

    stage = [0] * len(flows)
    placed = False
    for letter in "".join(ORDER):
        i = ord(letter) - ord("a")
        if stage[i] == 2 and not placed:
            state_windows()
            placed = True
        getattr(flows[i], STAGES[stage[i]])()
        stage[i] += 1

    def row_out(r, c):
        tile, at_row = lax.div(2 * pos[2] + r, 8), pl.ds(lax.rem(2 * pos[2] + r, 8), 1)
        for k in range(2):
            for win, out in ((m_win[k], new_m[k]), (v_win[k], new_v[k])):
                for layer in (0, 1):
                    out[r, pl.ds(layer, 1), :] = win[layer, tile, at_row, :]
        return c

    lax.fori_loop(0, 10, row_out, 0)
    for f in flows:
        f.done()
    for f in flows:
        for gather in (f.gather2, f.gather1):
            gather.wait_sent()


def solution(mesh):
    def step(*arrays):
        terms, weights, m, v = (arrays[i : i + 3] for i in (0, 3, 6, 9))
        shapes = ((2, 4, 4, 5, 8, 2048), (2, 4, 4, 5, 8, 2048), (2, 4, 4, 4, 4, 8, 640))
        terms = [t.reshape(s) for t, s in zip(terms, shapes, strict=True)]
        weights = [w.reshape(s) for w, s in zip(weights, shapes, strict=True)]

        def state_in(x):
            return x.transpose(1, 0, 2) if x.shape[1] == 10 else x.reshape(2, 4, 8, 640)

        m, v = [state_in(x) for x in m], [state_in(x) for x in v]
        state_shapes = [x.shape for x in m]
        outs = [(s, BF16) for s in shapes] + [(s, F32) for s in state_shapes] * 2
        scratch = [pltpu.VMEM(s, F32) for s in state_shapes] * 2
        scratch += [pltpu.VMEM((2, 2, 8, 2048), BF16)] * 2 + [pltpu.VMEM((2, 4, 8, 640), BF16)]
        scratch += [pltpu.VMEM((2, 2, 8, 2048), F32)] * 4
        scratch += [pltpu.VMEM(p.shape(p.lead1, 2), BF16) for p in PIECES[:3]]
        scratch += [pltpu.VMEM(s, d) for p in PIECES for s, d in p.scratch()]
        scratch += [pltpu.SemaphoreType.DMA((n,)) for n in (2 * len(PIECES), 7 * len(PIECES), LOADS)]
        new = pl.pallas_call(
            kernel,
            name="step",
            out_shape=[pltpu.VMEM(s, d) for s, d in outs],
            in_specs=[pl.BlockSpec(memory_space=pl.ANY)] * 12,
            out_specs=[pl.BlockSpec(memory_space=pltpu.VMEM)] * 9,
            scratch_shapes=scratch,
            compiler_params=pltpu.CompilerParams(collective_id=0, has_side_effects=True, vmem_limit_bytes=46 * 2**20),
        )(*terms, *weights, *m, *v)

        def put(*refs):
            sems = refs[18]
            copies = [pltpu.make_async_copy(refs[i], refs[9 + i], sems.at[i]) for i in range(9)]
            for copy in copies:
                copy.start()
            for copy in copies:
                copy.wait()

        new = pl.pallas_call(
            put,
            name="put",
            out_shape=[jax.ShapeDtypeStruct(s, d) for s, d in outs],
            in_specs=[pl.BlockSpec(memory_space=pltpu.VMEM)] * 9,
            out_specs=[pl.BlockSpec(memory_space=pl.ANY)] * 9,
            scratch_shapes=[pltpu.SemaphoreType.DMA((9,))],
            compiler_params=pltpu.CompilerParams(vmem_limit_bytes=2**20),
        )(*(pltpu.with_memory_space_constraint(x, pltpu.VMEM) for x in new))

        def state_out(x):
            return x.transpose(1, 0, 2) if x.shape[0] == 10 else x.reshape(2, 32, 640)

        whole = [w.reshape(s) for w, s in zip(new[:3], ((2, 640, 2048), (2, 640, 2048), (2, 2048, 640)), strict=True)]
        return (*whole, *(state_out(x) for x in new[3:]))

    all_of, cut = P(None, None, None), P(None, "dp", None)
    return jax.shard_map(
        step,
        mesh=mesh,
        in_specs=(P(("rep", "dp"), None, None, None),) * 3 + (all_of,) * 3 + (cut,) * 6,
        out_specs=(P("rep", None, None),) * 3 + (P("rep", "dp", None),) * 6,
        check_vma=False,
    )
```

```python
import jax
import jax.numpy as jnp
from jax import lax
from jax.experimental import pallas as pl
from jax.experimental.pallas import tpu as pltpu
from jax.sharding import PartitionSpec as P

STAGES = (
    *("far1", "near1", "relay1", "sum1", "relay2", "sum2", "relay3", "step"),
    *("forward3", "merge", "forward2", "out1", "rest1", "forward1"),
)
ORDER = (
    "abebheddcfacgfadcfiibeabjfhabgekdciehgcjbadfkklbchjgalfedabh",
    "lkcgdfjebchigdakfjelbghcadkfeijblghafkjcidlbhgkalijcfabekdaj",
    "ihgblckecichgljeeikffgidgjdlhillljfkdkghhijelkij",
)

MESH = pl.DeviceIdType.MESH
F32, BF16 = jnp.float32, jnp.bfloat16
CHUNKS = 4
COLS = 2048 // CHUNKS
EARLY = 1
TILES = 4 // CHUNKS


class Piece:
    def __init__(self, weight, chunk):
        self.weight, self.chunk = weight, chunk
        self.early = weight < 2 and chunk == EARLY
        if weight < 2:
            self.axes = ((0, 2, 1), (1, 2, 0))[weight] if self.early else ((0, 1, 2), (1, 0, 2))[weight]
            self.lead1, self.lead2, self.lead3 = (4, 5), (4, 2) if self.early else (5,), (2,)
            self.cols = COLS
        else:
            self.axes = ((2, 0, 1), (2, 1, 0))[chunk % 2]
            self.lead1, self.lead2, self.lead3 = (4, 4, TILES), (4, TILES), (TILES,)
            self.cols = 640

    def shape(self, lead, *front):
        return (*front, *lead, 8, self.cols)

    def scratch(self):
        one, two, three = self.lead1, self.lead2, self.lead3
        shapes = [
            (self.shape(one, 2, 2), BF16),
            (self.shape(one, 3, 2), BF16),
            (self.shape(two, 2, 2), F32),
            (self.shape(two, 2, 2), BF16),
            (self.shape(two, 3, 2), BF16),
            (self.shape(two, 2), F32),
            (self.shape(two, 2), BF16),
            (self.shape(three, 3, 2), BF16),
        ]
        if self.weight < 2:
            shapes.append((self.shape(two if self.early else three, 4, 2), BF16))
        return shapes

    def columns(self):
        return pl.ds(self.chunk * COLS, COLS)

    def first(self, ref, layer, p):
        if self.weight == 0:
            return ref.at[layer, p, :, :, :, self.columns()]
        if self.weight == 1:
            return ref.at[layer, :, p, :, :, self.columns()]
        return ref.at[layer, :, :, p, pl.ds(self.chunk * TILES, TILES)]

    def second(self, block, p):
        if self.early:
            return block.at[:, pl.ds(p, 2)]
        if self.weight == 2 and self.axes[1] == 1:
            return block.at[:, p]
        return block.at[p]

    def third(self, block, p):
        return block.at[p] if self.weight == 2 or self.early else block.at[pl.ds(p, 2)]

    def out2(self, ref, layer, p, pos):
        if self.weight == 0:
            return ref.at[layer, pos[0], p, :, :, self.columns()]
        if self.weight == 1:
            return ref.at[layer, p, pos[1], :, :, self.columns()]
        rows = pl.ds(self.chunk * TILES, TILES)
        if self.axes[1] == 0:
            return ref.at[layer, p, :, pos[2], rows]
        return ref.at[layer, :, p, pos[2], rows]

    def out3(self, ref, layer, p, pos):
        rows = pl.ds(self.chunk * TILES, TILES)
        if self.axes[2] == 1:
            return ref.at[layer, pos[0], p, pos[2], rows]
        return ref.at[layer, p, pos[1], pos[2], rows]


PIECES = [Piece(w, c) for c in range(CHUNKS) for w in range(3)]
LOADS = 2 * CHUNKS + 5

RECEIVES = ((0, 1), (2, 3), (4, 5), (4, 3), (2, 1), (0, 6))


def add_into(lead, terms, outs):
    def body(index):
        total = terms[0][index].astype(F32)
        for t in terms[1:]:
            total = total + t[index].astype(F32)
        for o in outs:
            o[index] = total.astype(o.dtype)

    if len(lead) > 2 or lead == (4, 5):
        lax.fori_loop(0, lead[0], lambda i, c: (body(i), c)[1], 0)
    else:
        body(...)


def adamw(w, m, v, g):
    m = 0.9 * m + 0.1 * g
    v = 0.95 * v + 0.05 * g * g
    step = m * lax.rsqrt(v + 1e-8) + 0.1 * w
    return w - 0.02 * step, m, v


def kernel(*refs):
    refs = list(refs)

    def take(n):
        got, refs[:n] = refs[:n], []
        return got

    grads, weights, ms, vs = take(3), take(3), take(3), take(3)
    new_w, new_m, new_v = take(3), take(3), take(3)
    m_in, v_in, w_in = take(3), take(3), take(3)
    m_win, v_win = take(2), take(2)
    ahead = take(3)
    bufs = [take(len(p.scratch())) for p in PIECES]
    send_sem, recv_sem, load_sem = take(3)

    me = lax.axis_index("dp")
    pos = (lax.div(me, 16), lax.rem(lax.div(me, 4), 4), lax.rem(me, 4))
    stride = (16, 4, 1)

    def at(axis, d):
        return lax.rem(pos[axis] + d, 4)

    def neighbour(axis, d):
        return me + (at(axis, d) - pos[axis]) * stride[axis]

    plus = [neighbour(a, 1) for a in range(3)]
    minus = [neighbour(a, 3) for a in range(3)]

    barrier = pltpu.get_barrier_semaphore()
    for other in (*plus, *minus):
        pl.semaphore_signal(barrier, inc=1, device_id={"dp": other}, device_id_type=MESH)

    def wait(sem, like):
        pltpu.make_async_copy(like, like, sem).wait()

    loaded = set()

    def load(src, dst, sem):
        pltpu.make_async_copy(src, dst, sem).start()

    class Move:
        def __init__(self, index, stage, axis, recv):
            self.axis, self.recv = axis, recv
            self.sent = send_sem.at[2 * index + stage % 2]
            self.sems = [7 * index + i for i in RECEIVES[stage]]

        def remote(self, src, dst, forward, first):
            pltpu.make_async_remote_copy(
                src_ref=src,
                dst_ref=dst,
                send_sem=self.sent,
                recv_sem=recv_sem.at[self.sems[0 if first else 1]],
                device_id={"dp": (plus if forward else minus)[self.axis]},
                device_id_type=MESH,
            ).start()

        def wait_first(self):
            wait(recv_sem.at[self.sems[0]], self.recv.at[0])

        def wait_rest(self):
            wait(recv_sem.at[self.sems[1]], self.recv.at[pl.ds(1, 2)])

        def wait_sent(self):
            wait(self.sent, self.recv)

    class Scatter(Move):
        def __init__(self, index, stage, axis, recv, far, near, lead, relay_term):
            super().__init__(index, stage, axis, recv)
            self.far, self.near, self.lead, self.relay_term = far, near, lead, relay_term

        def send_far(self):
            for layer in (0, 1):
                self.remote(self.far(layer), self.recv.at[0, layer], layer == 0, True)

        def send_near(self):
            for layer in (1, 0):
                self.remote(self.near(layer), self.recv.at[1, layer], layer == 1, False)

        def relay(self):
            self.wait_first()
            for layer in (0, 1):
                here = self.recv.at[0, layer]
                add_into(self.lead, (here, self.relay_term(layer)), (here,))
                self.remote(here, self.recv.at[2, layer], layer == 0, False)

    class Gather(Move):
        def __init__(self, index, stage, scatter, block):
            super().__init__(index, stage, scatter.axis, scatter.recv)
            self.block = block

        def send(self, layer, p, forward, first):
            ref = self.block(layer, p)
            self.remote(ref, ref, forward, first)

        def start(self):
            mine = pos[self.axis]
            self.send(0, mine, True, True)
            self.send(1, mine, False, True)

        def start_rest(self):
            mine = pos[self.axis]
            self.send(1, mine, True, False)
            self.send(0, mine, False, False)

        def forward(self):
            self.wait_first()
            self.send(0, at(self.axis, 3), True, False)
            self.send(1, at(self.axis, 1), False, False)

    class Flow:
        def __init__(self, index, piece, buf):
            self.piece, self.buf = piece, buf
            a1, a2, a3 = piece.axes
            g = grads[piece.weight]
            own1, recv1, sum1, send1, recv2, sum2, send2, recv3 = buf[:8]
            self.scatter1 = Scatter(
                index,
                0,
                a1,
                recv1,
                lambda layer: piece.first(g, layer, at(a1, 2)) if piece.chunk else ahead[piece.weight].at[layer],
                lambda layer: piece.first(g, layer, at(a1, 1 if layer else 3)),
                piece.lead1,
                lambda layer: own1.at[layer, 1],
            )
            self.scatter2 = Scatter(
                index,
                1,
                a2,
                recv2,
                lambda layer: send1.at[layer, 0],
                lambda layer: send1.at[layer, 1],
                piece.lead2,
                lambda layer: sum1.at[layer, 1],
            )
            self.scatter3 = Scatter(
                index,
                2,
                a3,
                recv3,
                lambda layer: piece.third(send2.at[layer], at(a3, 2)),
                lambda layer: piece.third(send2.at[layer], at(a3, 1 if layer else 3)),
                piece.lead3,
                lambda layer: piece.third(sum2.at[layer], at(a3, 3 if layer else 1)),
            )
            w = new_w[piece.weight]
            if piece.weight < 2:
                windows = buf[8]
                if piece.early:
                    self.gather3 = Gather(index, 3, self.scatter3, lambda layer, p: windows.at[pos[2], layer, p])
                else:
                    self.gather3 = Gather(index, 3, self.scatter3, lambda layer, p: windows.at[p, layer])
            else:
                self.gather3 = Gather(index, 3, self.scatter3, lambda layer, p: piece.out3(w, layer, p, pos))
            if piece.early:
                self.gather2 = Gather(index, 4, self.scatter2, lambda layer, p: windows.at[p, layer])
            else:
                self.gather2 = Gather(index, 4, self.scatter2, lambda layer, p: piece.out2(w, layer, p, pos))
            self.gather1 = Gather(index, 5, self.scatter1, lambda layer, p: piece.first(w, layer, p))

        def load(self):
            piece, own1 = self.piece, self.buf[0]
            a1, g = piece.axes[0], grads[piece.weight]
            for which in (1, 0):
                for layer in (0, 1):
                    p = at(a1, (3 if layer else 1) if which else 0)
                    load(piece.first(g, layer, p), own1.at[layer, which], load_sem.at[2 * piece.chunk + which])

        def wait_load(self, which):
            i = 2 * self.piece.chunk + which
            if i not in loaded:
                loaded.add(i)
                wait(load_sem.at[i], self.buf[1])

        def far1(self):
            self.scatter1.send_far()

        def near1(self):
            self.scatter1.send_near()

        def relay1(self):
            self.wait_load(1)
            self.scatter1.relay()

        def sum1(self):
            piece = self.piece
            own1, recv1, sum1, send1 = self.buf[:4]
            a2 = piece.axes[1]
            self.wait_load(0)
            self.scatter1.wait_rest()

            def reduce(layer, d, out):
                p = at(a2, d)
                terms = (own1.at[layer, 0], recv1.at[1, layer], recv1.at[2, layer])
                add_into(piece.lead2, [piece.second(t, p) for t in terms], (out,))

            for layer in (0, 1):
                reduce(layer, 2, send1.at[layer, 0])
            self.scatter2.send_far()
            for layer in (1, 0):
                reduce(layer, 1 if layer else 3, send1.at[layer, 1])
            self.scatter2.send_near()
            for layer in (0, 1):
                reduce(layer, 3 if layer else 1, sum1.at[layer, 1])
            for layer in (0, 1):
                reduce(layer, 0, sum1.at[layer, 0])

        def relay2(self):
            self.scatter2.relay()

        def sum2(self):
            sum1, _, recv2, sum2, send2 = self.buf[2:7]
            self.scatter2.wait_rest()
            for layer in (0, 1):
                terms = (sum1.at[layer, 0], recv2.at[1, layer], recv2.at[2, layer])
                add_into(self.piece.lead2, terms, (sum2.at[layer], send2.at[layer]))
            self.scatter1.wait_sent()
            self.scatter3.send_far()
            self.scatter3.send_near()

        def relay3(self):
            self.scatter3.relay()

        def step(self):
            piece = self.piece
            sum2, recv3 = self.buf[5], self.buf[7]
            a3, k = piece.axes[2], piece.weight
            self.scatter3.wait_rest()
            for layer in (0, 1):
                terms = (piece.third(sum2.at[layer], pos[a3]), recv3.at[1, layer], recv3.at[2, layer])
                g = terms[0][...] + terms[1][...].astype(F32) + terms[2][...].astype(F32)
                g = g.astype(BF16).astype(F32)
                if k < 2:
                    cols = piece.columns()
                    w, m, v = w_in[k][layer, :, :, cols].astype(F32), m_win[k][layer, :, :, cols], v_win[k][layer, :, :, cols]
                    w, m, v = adamw(w, m, v, g)
                    m_win[k][layer, :, :, cols] = m
                    v_win[k][layer, :, :, cols] = v
                    row = lax.broadcasted_iota(jnp.int32, w.shape, 1) + 8 * lax.broadcasted_iota(jnp.int32, w.shape, 0)
                    mine = (row >= 2 * pos[2]) & (row < 2 * pos[2] + 10)
                    windows = self.gather3.block(layer, pos[a3])
                    windows[...] = jnp.where(mine, w, 0.0).astype(BF16)
                else:
                    t = pl.ds(piece.chunk * TILES, TILES)
                    w, m, v = adamw(w_in[k][layer, t].astype(F32), m_in[k][layer, t], v_in[k][layer, t], g)
                    new_m[k][layer, t] = m
                    new_v[k][layer, t] = v
                    new_w[k][layer, pos[0], pos[1], pos[2], t] = w.astype(BF16)
            self.scatter2.wait_sent()
            self.gather3.start()
            self.gather3.start_rest()

        def forward3(self):
            self.gather3.forward()

        def merge(self):
            self.gather3.wait_rest()
            if self.piece.weight < 2 and not self.piece.early:
                self.join(lambda t: (pos[self.piece.axes[1]], t))
            self.scatter3.wait_sent()
            self.gather2.start()
            self.gather2.start_rest()

        def join(self, tile):
            piece, windows = self.piece, self.buf[8]
            for layer in (0, 1):
                out = piece.first(new_w[piece.weight], layer, pos[piece.axes[0]])
                part = [windows.at[z, layer, :, j] if piece.early else windows.at[z, layer, j] for z in range(4) for j in (0, 1)]
                out[tile(0)] = part[0][...]
                for t in (1, 2, 3):
                    out[tile(t)] = (part[2 * t - 1][...].astype(F32) + part[2 * t][...].astype(F32)).astype(BF16)
                out[tile(4)] = part[7][...]

        def forward2(self):
            self.gather2.forward()

        def out1(self):
            self.gather2.wait_rest()
            if self.piece.early:
                self.join(lambda t: (slice(None), t))
            self.gather3.wait_sent()
            self.gather1.start()

        def rest1(self):
            self.gather1.start_rest()

        def forward1(self):
            self.gather1.forward()

        def done(self):
            self.gather1.wait_rest()

    flows = [Flow(i, p, b) for i, (p, b) in enumerate(zip(PIECES, bufs, strict=True))]
    for f, dst in zip(flows, ahead, strict=False):
        for layer in (0, 1):
            load(f.piece.first(grads[f.piece.weight], layer, at(f.piece.axes[0], 2)), dst.at[layer], load_sem.at[LOADS - 1])
    for f in flows:
        f.load()
    state_sem = 2 * CHUNKS
    for k in range(3):
        own = weights[k].at[:, pos[0], pos[1], pl.ds(pos[2], 2)] if k < 2 else weights[k].at[:, pos[0], pos[1], pos[2]]
        load(own, w_in[k], load_sem.at[state_sem + 1 + k])
        load(ms[k], m_in[k], load_sem.at[state_sem])
        load(vs[k], v_in[k], load_sem.at[state_sem])
    wait(load_sem.at[LOADS - 1], bufs[0][1])
    pl.semaphore_wait(barrier, 6)

    def state_windows():
        wait(load_sem.at[state_sem], bufs[0][1])
        for k in range(3):
            wait(load_sem.at[state_sem + 1 + k], w_in[k])
        for k in range(2):
            for win in (m_win[k], v_win[k]):
                win[...] = jnp.zeros_like(win)

        def row(r, c):
            tile, at_row = lax.div(2 * pos[2] + r, 8), pl.ds(lax.rem(2 * pos[2] + r, 8), 1)
            for k in range(2):
                for win, data in ((m_win[k], m_in[k]), (v_win[k], v_in[k])):
                    for layer in (0, 1):
                        win[layer, tile, at_row, :] = data[r, pl.ds(layer, 1), :]
            return c

        lax.fori_loop(0, 10, row, 0)

    stage = [0] * len(flows)
    placed = False
    for letter in "".join(ORDER):
        i = ord(letter) - ord("a")
        if stage[i] == 2 and not placed:
            state_windows()
            placed = True
        getattr(flows[i], STAGES[stage[i]])()
        stage[i] += 1

    def row_out(r, c):
        tile, at_row = lax.div(2 * pos[2] + r, 8), pl.ds(lax.rem(2 * pos[2] + r, 8), 1)
        for k in range(2):
            for win, out in ((m_win[k], new_m[k]), (v_win[k], new_v[k])):
                for layer in (0, 1):
                    out[r, pl.ds(layer, 1), :] = win[layer, tile, at_row, :]
        return c

    lax.fori_loop(0, 10, row_out, 0)
    for f in flows:
        f.done()
    for f in flows:
        for gather in (f.gather2, f.gather1):
            gather.wait_sent()


def solution(mesh):
    def step(*arrays):
        terms, weights, m, v = (arrays[i : i + 3] for i in (0, 3, 6, 9))
        shapes = ((2, 4, 4, 5, 8, 2048), (2, 4, 4, 5, 8, 2048), (2, 4, 4, 4, 4, 8, 640))
        terms = [t.reshape(s) for t, s in zip(terms, shapes, strict=True)]
        weights = [w.reshape(s) for w, s in zip(weights, shapes, strict=True)]

        def state_in(x):
            return x.transpose(1, 0, 2) if x.shape[1] == 10 else x.reshape(2, 4, 8, 640)

        m, v = [state_in(x) for x in m], [state_in(x) for x in v]
        state_shapes = [x.shape for x in m]
        outs = [(s, BF16) for s in shapes] + [(s, F32) for s in state_shapes] * 2
        scratch = [pltpu.VMEM(s, F32) for s in state_shapes] * 2
        scratch += [pltpu.VMEM((2, 2, 8, 2048), BF16)] * 2 + [pltpu.VMEM((2, 4, 8, 640), BF16)]
        scratch += [pltpu.VMEM((2, 2, 8, 2048), F32)] * 4
        scratch += [pltpu.VMEM(p.shape(p.lead1, 2), BF16) for p in PIECES[:3]]
        scratch += [pltpu.VMEM(s, d) for p in PIECES for s, d in p.scratch()]
        scratch += [pltpu.SemaphoreType.DMA((n,)) for n in (2 * len(PIECES), 7 * len(PIECES), LOADS)]
        new = pl.pallas_call(
            kernel,
            name="step",
            out_shape=[pltpu.VMEM(s, d) for s, d in outs],
            in_specs=[pl.BlockSpec(memory_space=pl.ANY)] * 12,
            out_specs=[pl.BlockSpec(memory_space=pltpu.VMEM)] * 9,
            scratch_shapes=scratch,
            compiler_params=pltpu.CompilerParams(collective_id=0, has_side_effects=True, vmem_limit_bytes=46 * 2**20),
        )(*terms, *weights, *m, *v)

        def put(*refs):
            sems = refs[18]
            copies = [pltpu.make_async_copy(refs[i], refs[9 + i], sems.at[i]) for i in range(9)]
            for copy in copies:
                copy.start()
            for copy in copies:
                copy.wait()

        new = pl.pallas_call(
            put,
            name="put",
            out_shape=[jax.ShapeDtypeStruct(s, d) for s, d in outs],
            in_specs=[pl.BlockSpec(memory_space=pltpu.VMEM)] * 9,
            out_specs=[pl.BlockSpec(memory_space=pl.ANY)] * 9,
            scratch_shapes=[pltpu.SemaphoreType.DMA((9,))],
            compiler_params=pltpu.CompilerParams(vmem_limit_bytes=2**20),
        )(*(pltpu.with_memory_space_constraint(x, pltpu.VMEM) for x in new))

        def state_out(x):
            return x.transpose(1, 0, 2) if x.shape[0] == 10 else x.reshape(2, 32, 640)

        whole = [w.reshape(s) for w, s in zip(new[:3], ((2, 640, 2048), (2, 640, 2048), (2, 2048, 640)), strict=True)]
        return (*whole, *(state_out(x) for x in new[3:]))

    all_of, cut = P(None, None, None), P(None, "dp", None)
    return jax.shard_map(
        step,
        mesh=mesh,
        in_specs=(P(("rep", "dp"), None, None, None),) * 3 + (all_of,) * 3 + (cut,) * 6,
        out_specs=(P("rep", None, None),) * 3 + (P("rep", "dp", None),) * 6,
        check_vma=False,
    )
```

```python
import jax
import jax.numpy as jnp
from jax import lax
from jax.experimental import pallas as pl
from jax.experimental.pallas import tpu as pltpu
from jax.sharding import PartitionSpec as P

STAGES = (
    *("far1", "near1", "relay1", "sum1", "relay2", "sum2", "relay3", "step"),
    *("forward3", "merge", "forward2", "out1", "rest1", "forward1"),
)
ORDER = (
    "abebheddcfacgfadcfiibeabjfhabgekdciehgcjbadfkklbchjgalfedabh",
    "lkcgdfjebchigdakfjelbghcadkfeijblghafkjcidlbhgkalijcfabekdaj",
    "ihgblckecichgljeeikffgidgjdlhillljfkdkghhijelkij",
)

MESH = pl.DeviceIdType.MESH
F32, BF16 = jnp.float32, jnp.bfloat16
CHUNKS = 4
COLS = 2048 // CHUNKS
EARLY = 1
TILES = 4 // CHUNKS


class Piece:
    def __init__(self, weight, chunk):
        self.weight, self.chunk = weight, chunk
        self.early = weight < 2 and chunk == EARLY
        if weight < 2:
            self.axes = ((0, 2, 1), (1, 2, 0))[weight] if self.early else ((0, 1, 2), (1, 0, 2))[weight]
            self.lead1, self.lead2, self.lead3 = (4, 5), (4, 2) if self.early else (5,), (2,)
            self.cols = COLS
        else:
            self.axes = ((2, 0, 1), (2, 1, 0))[chunk % 2]
            self.lead1, self.lead2, self.lead3 = (4, 4, TILES), (4, TILES), (TILES,)
            self.cols = 640

    def shape(self, lead, *front):
        return (*front, *lead, 8, self.cols)

    def scratch(self):
        one, two, three = self.lead1, self.lead2, self.lead3
        shapes = [
            (self.shape(one, 2, 2), BF16),
            (self.shape(one, 3, 2), BF16),
            (self.shape(two, 2, 2), F32),
            (self.shape(two, 2, 2), BF16),
            (self.shape(two, 3, 2), BF16),
            (self.shape(two, 2), F32),
            (self.shape(two, 2), BF16),
            (self.shape(three, 3, 2), BF16),
        ]
        if self.weight < 2:
            shapes.append((self.shape(two if self.early else three, 4, 2), BF16))
        return shapes

    def columns(self):
        return pl.ds(self.chunk * COLS, COLS)

    def first(self, ref, layer, p):
        if self.weight == 0:
            return ref.at[layer, p, :, :, :, self.columns()]
        if self.weight == 1:
            return ref.at[layer, :, p, :, :, self.columns()]
        return ref.at[layer, :, :, p, pl.ds(self.chunk * TILES, TILES)]

    def second(self, block, p):
        if self.early:
            return block.at[:, pl.ds(p, 2)]
        if self.weight == 2 and self.axes[1] == 1:
            return block.at[:, p]
        return block.at[p]

    def third(self, block, p):
        return block.at[p] if self.weight == 2 or self.early else block.at[pl.ds(p, 2)]

    def out2(self, ref, layer, p, pos):
        if self.weight == 0:
            return ref.at[layer, pos[0], p, :, :, self.columns()]
        if self.weight == 1:
            return ref.at[layer, p, pos[1], :, :, self.columns()]
        rows = pl.ds(self.chunk * TILES, TILES)
        if self.axes[1] == 0:
            return ref.at[layer, p, :, pos[2], rows]
        return ref.at[layer, :, p, pos[2], rows]

    def out3(self, ref, layer, p, pos):
        rows = pl.ds(self.chunk * TILES, TILES)
        if self.axes[2] == 1:
            return ref.at[layer, pos[0], p, pos[2], rows]
        return ref.at[layer, p, pos[1], pos[2], rows]


PIECES = [Piece(w, c) for c in range(CHUNKS) for w in range(3)]
LOADS = CHUNKS + 5

RECEIVES = ((0, 1), (2, 3), (4, 5), (4, 3), (2, 1), (0, 6))


def add_into(lead, terms, outs):
    def body(index):
        total = terms[0][index].astype(F32)
        for t in terms[1:]:
            total = total + t[index].astype(F32)
        for o in outs:
            o[index] = total.astype(o.dtype)

    if len(lead) > 2 or lead == (4, 5):
        lax.fori_loop(0, lead[0], lambda i, c: (body(i), c)[1], 0)
    else:
        body(...)


def adamw(w, m, v, g):
    m = 0.9 * m + 0.1 * g
    v = 0.95 * v + 0.05 * g * g
    step = m * lax.rsqrt(v + 1e-8) + 0.1 * w
    return w - 0.02 * step, m, v


def kernel(*refs):
    refs = list(refs)

    def take(n):
        got, refs[:n] = refs[:n], []
        return got

    grads, weights, ms, vs = take(3), take(3), take(3), take(3)
    new_w, new_m, new_v = take(3), take(3), take(3)
    m_in, v_in, w_in = take(3), take(3), take(3)
    m_win, v_win = take(2), take(2)
    ahead = take(3)
    bufs = [take(len(p.scratch())) for p in PIECES]
    send_sem, recv_sem, load_sem = take(3)

    me = lax.axis_index("dp")
    pos = (lax.div(me, 16), lax.rem(lax.div(me, 4), 4), lax.rem(me, 4))
    stride = (16, 4, 1)

    def at(axis, d):
        return lax.rem(pos[axis] + d, 4)

    def neighbour(axis, d):
        return me + (at(axis, d) - pos[axis]) * stride[axis]

    plus = [neighbour(a, 1) for a in range(3)]
    minus = [neighbour(a, 3) for a in range(3)]

    barrier = pltpu.get_barrier_semaphore()
    for other in (*plus, *minus):
        pl.semaphore_signal(barrier, inc=1, device_id={"dp": other}, device_id_type=MESH)

    def wait(sem, like):
        pltpu.make_async_copy(like, like, sem).wait()

    loaded = set()

    def load(src, dst, sem):
        pltpu.make_async_copy(src, dst, sem).start()

    class Move:
        def __init__(self, index, stage, axis, recv):
            self.axis, self.recv = axis, recv
            self.sent = send_sem.at[2 * index + stage % 2]
            self.sems = [7 * index + i for i in RECEIVES[stage]]

        def remote(self, src, dst, forward, first):
            pltpu.make_async_remote_copy(
                src_ref=src,
                dst_ref=dst,
                send_sem=self.sent,
                recv_sem=recv_sem.at[self.sems[0 if first else 1]],
                device_id={"dp": (plus if forward else minus)[self.axis]},
                device_id_type=MESH,
            ).start()

        def wait_first(self):
            wait(recv_sem.at[self.sems[0]], self.recv.at[0])

        def wait_rest(self):
            wait(recv_sem.at[self.sems[1]], self.recv.at[pl.ds(1, 2)])

        def wait_sent(self):
            wait(self.sent, self.recv)

    class Scatter(Move):
        def __init__(self, index, stage, axis, recv, far, near, lead, relay_term):
            super().__init__(index, stage, axis, recv)
            self.far, self.near, self.lead, self.relay_term = far, near, lead, relay_term

        def send_far(self):
            for layer in (0, 1):
                self.remote(self.far(layer), self.recv.at[0, layer], layer == 0, True)

        def send_near(self):
            for layer in (1, 0):
                self.remote(self.near(layer), self.recv.at[1, layer], layer == 1, False)

        def relay(self):
            self.wait_first()
            for layer in (0, 1):
                here = self.recv.at[0, layer]
                add_into(self.lead, (here, self.relay_term(layer)), (here,))
                self.remote(here, self.recv.at[2, layer], layer == 0, False)

    class Gather(Move):
        def __init__(self, index, stage, scatter, block):
            super().__init__(index, stage, scatter.axis, scatter.recv)
            self.block = block

        def send(self, layer, p, forward, first):
            ref = self.block(layer, p)
            self.remote(ref, ref, forward, first)

        def start(self):
            mine = pos[self.axis]
            self.send(0, mine, True, True)
            self.send(1, mine, False, True)

        def start_rest(self):
            mine = pos[self.axis]
            self.send(1, mine, True, False)
            self.send(0, mine, False, False)

        def forward(self):
            self.wait_first()
            self.send(0, at(self.axis, 3), True, False)
            self.send(1, at(self.axis, 1), False, False)

    class Flow:
        def __init__(self, index, piece, buf):
            self.piece, self.buf = piece, buf
            a1, a2, a3 = piece.axes
            g = grads[piece.weight]
            own1, recv1, sum1, send1, recv2, sum2, send2, recv3 = buf[:8]
            self.scatter1 = Scatter(
                index,
                0,
                a1,
                recv1,
                lambda layer: piece.first(g, layer, at(a1, 2)) if piece.chunk else ahead[piece.weight].at[layer],
                lambda layer: piece.first(g, layer, at(a1, 1 if layer else 3)),
                piece.lead1,
                lambda layer: own1.at[layer, 1],
            )
            self.scatter2 = Scatter(
                index,
                1,
                a2,
                recv2,
                lambda layer: send1.at[layer, 0],
                lambda layer: send1.at[layer, 1],
                piece.lead2,
                lambda layer: sum1.at[layer, 1],
            )
            self.scatter3 = Scatter(
                index,
                2,
                a3,
                recv3,
                lambda layer: piece.third(send2.at[layer], at(a3, 2)),
                lambda layer: piece.third(send2.at[layer], at(a3, 1 if layer else 3)),
                piece.lead3,
                lambda layer: piece.third(sum2.at[layer], at(a3, 3 if layer else 1)),
            )
            w = new_w[piece.weight]
            if piece.weight < 2:
                windows = buf[8]
                if piece.early:
                    self.gather3 = Gather(index, 3, self.scatter3, lambda layer, p: windows.at[pos[2], layer, p])
                else:
                    self.gather3 = Gather(index, 3, self.scatter3, lambda layer, p: windows.at[p, layer])
            else:
                self.gather3 = Gather(index, 3, self.scatter3, lambda layer, p: piece.out3(w, layer, p, pos))
            if piece.early:
                self.gather2 = Gather(index, 4, self.scatter2, lambda layer, p: windows.at[p, layer])
            else:
                self.gather2 = Gather(index, 4, self.scatter2, lambda layer, p: piece.out2(w, layer, p, pos))
            self.gather1 = Gather(index, 5, self.scatter1, lambda layer, p: piece.first(w, layer, p))

        def load(self):
            piece, own1 = self.piece, self.buf[0]
            a1, g = piece.axes[0], grads[piece.weight]
            for which in (1, 0):
                for layer in (0, 1):
                    p = at(a1, (3 if layer else 1) if which else 0)
                    load(piece.first(g, layer, p), own1.at[layer, which], load_sem.at[piece.chunk])

        def wait_load(self):
            i = self.piece.chunk
            if i not in loaded:
                loaded.add(i)
                wait(load_sem.at[i], grads[0].at[:, :3, :2])

        def far1(self):
            self.scatter1.send_far()

        def near1(self):
            self.scatter1.send_near()

        def relay1(self):
            self.wait_load()
            self.scatter1.relay()

        def sum1(self):
            piece = self.piece
            own1, recv1, sum1, send1 = self.buf[:4]
            a2 = piece.axes[1]
            self.scatter1.wait_rest()

            def reduce(layer, d, out):
                p = at(a2, d)
                terms = (own1.at[layer, 0], recv1.at[1, layer], recv1.at[2, layer])
                add_into(piece.lead2, [piece.second(t, p) for t in terms], (out,))

            for layer in (0, 1):
                reduce(layer, 2, send1.at[layer, 0])
            self.scatter2.send_far()
            for layer in (1, 0):
                reduce(layer, 1 if layer else 3, send1.at[layer, 1])
            self.scatter2.send_near()
            for layer in (0, 1):
                reduce(layer, 3 if layer else 1, sum1.at[layer, 1])
            for layer in (0, 1):
                reduce(layer, 0, sum1.at[layer, 0])

        def relay2(self):
            self.scatter2.relay()

        def sum2(self):
            sum1, _, recv2, sum2, send2 = self.buf[2:7]
            self.scatter2.wait_rest()
            for layer in (0, 1):
                terms = (sum1.at[layer, 0], recv2.at[1, layer], recv2.at[2, layer])
                add_into(self.piece.lead2, terms, (sum2.at[layer], send2.at[layer]))
            self.scatter1.wait_sent()
            self.scatter3.send_far()
            self.scatter3.send_near()

        def relay3(self):
            self.scatter3.relay()

        def step(self):
            piece = self.piece
            sum2, recv3 = self.buf[5], self.buf[7]
            a3, k = piece.axes[2], piece.weight
            self.scatter3.wait_rest()
            for layer in (0, 1):
                terms = (piece.third(sum2.at[layer], pos[a3]), recv3.at[1, layer], recv3.at[2, layer])
                g = terms[0][...] + terms[1][...].astype(F32) + terms[2][...].astype(F32)
                g = g.astype(BF16).astype(F32)
                if k < 2:
                    cols = piece.columns()
                    w, m, v = w_in[k][layer, :, :, cols].astype(F32), m_win[k][layer, :, :, cols], v_win[k][layer, :, :, cols]
                    w, m, v = adamw(w, m, v, g)
                    m_win[k][layer, :, :, cols] = m
                    v_win[k][layer, :, :, cols] = v
                    row = lax.broadcasted_iota(jnp.int32, w.shape, 1) + 8 * lax.broadcasted_iota(jnp.int32, w.shape, 0)
                    mine = (row >= 2 * pos[2]) & (row < 2 * pos[2] + 10)
                    windows = self.gather3.block(layer, pos[a3])
                    windows[...] = jnp.where(mine, w, 0.0).astype(BF16)
                else:
                    t = pl.ds(piece.chunk * TILES, TILES)
                    w, m, v = adamw(w_in[k][layer, t].astype(F32), m_in[k][layer, t], v_in[k][layer, t], g)
                    new_m[k][layer, t] = m
                    new_v[k][layer, t] = v
                    new_w[k][layer, pos[0], pos[1], pos[2], t] = w.astype(BF16)
            self.scatter2.wait_sent()
            self.gather3.start()
            self.gather3.start_rest()

        def forward3(self):
            self.gather3.forward()

        def merge(self):
            self.gather3.wait_rest()
            if self.piece.weight < 2 and not self.piece.early:
                self.join(lambda t: (pos[self.piece.axes[1]], t))
            self.scatter3.wait_sent()
            self.gather2.start()
            self.gather2.start_rest()

        def join(self, tile):
            piece, windows = self.piece, self.buf[8]
            for layer in (0, 1):
                out = piece.first(new_w[piece.weight], layer, pos[piece.axes[0]])
                part = [windows.at[z, layer, :, j] if piece.early else windows.at[z, layer, j] for z in range(4) for j in (0, 1)]
                out[tile(0)] = part[0][...]
                for t in (1, 2, 3):
                    out[tile(t)] = (part[2 * t - 1][...].astype(F32) + part[2 * t][...].astype(F32)).astype(BF16)
                out[tile(4)] = part[7][...]

        def forward2(self):
            self.gather2.forward()

        def out1(self):
            self.gather2.wait_rest()
            if self.piece.early:
                self.join(lambda t: (slice(None), t))
            self.gather3.wait_sent()
            self.gather1.start()

        def rest1(self):
            self.gather1.start_rest()

        def forward1(self):
            self.gather1.forward()

        def done(self):
            self.gather1.wait_rest()

    flows = [Flow(i, p, b) for i, (p, b) in enumerate(zip(PIECES, bufs, strict=True))]
    for f, dst in zip(flows, ahead, strict=False):
        for layer in (0, 1):
            load(f.piece.first(grads[f.piece.weight], layer, at(f.piece.axes[0], 2)), dst.at[layer], load_sem.at[LOADS - 1])
    for f in flows:
        f.load()
    state_sem = CHUNKS
    for k in range(3):
        own = weights[k].at[:, pos[0], pos[1], pl.ds(pos[2], 2)] if k < 2 else weights[k].at[:, pos[0], pos[1], pos[2]]
        load(own, w_in[k], load_sem.at[state_sem + 1 + k])
        load(ms[k], m_in[k], load_sem.at[state_sem])
        load(vs[k], v_in[k], load_sem.at[state_sem])
    wait(load_sem.at[LOADS - 1], bufs[0][1])
    pl.semaphore_wait(barrier, 6)

    def state_windows():
        wait(load_sem.at[state_sem], bufs[0][1])
        for k in range(3):
            wait(load_sem.at[state_sem + 1 + k], w_in[k])
        for k in range(2):
            for win in (m_win[k], v_win[k]):
                win[...] = jnp.zeros_like(win)

        def row(r, c):
            tile, at_row = lax.div(2 * pos[2] + r, 8), pl.ds(lax.rem(2 * pos[2] + r, 8), 1)
            for k in range(2):
                for win, data in ((m_win[k], m_in[k]), (v_win[k], v_in[k])):
                    for layer in (0, 1):
                        win[layer, tile, at_row, :] = data[r, pl.ds(layer, 1), :]
            return c

        lax.fori_loop(0, 10, row, 0)

    stage = [0] * len(flows)
    placed = False
    for letter in "".join(ORDER):
        i = ord(letter) - ord("a")
        if stage[i] == 2 and not placed:
            state_windows()
            placed = True
        getattr(flows[i], STAGES[stage[i]])()
        stage[i] += 1

    def row_out(r, c):
        tile, at_row = lax.div(2 * pos[2] + r, 8), pl.ds(lax.rem(2 * pos[2] + r, 8), 1)
        for k in range(2):
            for win, out in ((m_win[k], new_m[k]), (v_win[k], new_v[k])):
                for layer in (0, 1):
                    out[r, pl.ds(layer, 1), :] = win[layer, tile, at_row, :]
        return c

    lax.fori_loop(0, 10, row_out, 0)
    whole_order = "".join(ORDER)
    for i in sorted(range(len(flows)), key=lambda i: whole_order.rindex(chr(ord("a") + i))):
        flows[i].done()
        flows[i].gather2.wait_sent()
        flows[i].gather1.wait_sent()


def solution(mesh):
    def step(*arrays):
        terms, weights, m, v = (arrays[i : i + 3] for i in (0, 3, 6, 9))
        shapes = ((2, 4, 4, 5, 8, 2048), (2, 4, 4, 5, 8, 2048), (2, 4, 4, 4, 4, 8, 640))
        terms = [t.reshape(s) for t, s in zip(terms, shapes, strict=True)]
        weights = [w.reshape(s) for w, s in zip(weights, shapes, strict=True)]

        def state_in(x):
            return x.transpose(1, 0, 2) if x.shape[1] == 10 else x.reshape(2, 4, 8, 640)

        m, v = [state_in(x) for x in m], [state_in(x) for x in v]
        state_shapes = [x.shape for x in m]
        outs = [(s, BF16) for s in shapes] + [(s, F32) for s in state_shapes] * 2
        scratch = [pltpu.VMEM(s, F32) for s in state_shapes] * 2
        scratch += [pltpu.VMEM((2, 2, 8, 2048), BF16)] * 2 + [pltpu.VMEM((2, 4, 8, 640), BF16)]
        scratch += [pltpu.VMEM((2, 2, 8, 2048), F32)] * 4
        scratch += [pltpu.VMEM(p.shape(p.lead1, 2), BF16) for p in PIECES[:3]]
        scratch += [pltpu.VMEM(s, d) for p in PIECES for s, d in p.scratch()]
        scratch += [pltpu.SemaphoreType.DMA((n,)) for n in (2 * len(PIECES), 7 * len(PIECES), LOADS)]
        new = pl.pallas_call(
            kernel,
            name="step",
            out_shape=[pltpu.VMEM(s, d) for s, d in outs],
            in_specs=[pl.BlockSpec(memory_space=pl.ANY)] * 12,
            out_specs=[pl.BlockSpec(memory_space=pltpu.VMEM)] * 9,
            scratch_shapes=scratch,
            compiler_params=pltpu.CompilerParams(collective_id=0, has_side_effects=True, vmem_limit_bytes=46 * 2**20),
        )(*terms, *weights, *m, *v)

        def put(*refs):
            sems = refs[18]
            copies = [pltpu.make_async_copy(refs[i], refs[9 + i], sems.at[min(i, 3)]) for i in range(9)]
            for copy in copies:
                copy.start()
            for copy in copies[:3]:
                copy.wait()
            moments = refs[0].at[:, 0, :3]
            pltpu.make_async_copy(moments, moments, sems.at[3]).wait()

        new = pl.pallas_call(
            put,
            name="put",
            out_shape=[jax.ShapeDtypeStruct(s, d) for s, d in outs],
            in_specs=[pl.BlockSpec(memory_space=pltpu.VMEM)] * 9,
            out_specs=[pl.BlockSpec(memory_space=pl.ANY)] * 9,
            scratch_shapes=[pltpu.SemaphoreType.DMA((4,))],
            compiler_params=pltpu.CompilerParams(vmem_limit_bytes=2**20),
        )(*(pltpu.with_memory_space_constraint(x, pltpu.VMEM) for x in new))

        def state_out(x):
            return x.transpose(1, 0, 2) if x.shape[0] == 10 else x.reshape(2, 32, 640)

        whole = [w.reshape(s) for w, s in zip(new[:3], ((2, 640, 2048), (2, 640, 2048), (2, 2048, 640)), strict=True)]
        return (*whole, *(state_out(x) for x in new[3:]))

    all_of, cut = P(None, None, None), P(None, "dp", None)
    return jax.shard_map(
        step,
        mesh=mesh,
        in_specs=(P(("rep", "dp"), None, None, None),) * 3 + (all_of,) * 3 + (cut,) * 6,
        out_specs=(P("rep", None, None),) * 3 + (P("rep", "dp", None),) * 6,
        check_vma=False,
    )
```
